256 devices in a mesh: gx: 16 (over z, x_lo), gy: 4 (over x_hi, core), gz: 4 (over y).
Axes of the slice: x: 4 (x_hi: 2, x_lo: 2; x = x_hi * 2 + x_lo), y: 4, z: 8, core: 2. Of those that a mesh axis runs over, the one named last changes fastest.
Arguments:
- velocity: float32 [3, 256, 64, 1024], P(None, 'gx', 'gy', 'gz'), may hold values from -24 to 24
- metric: float32 [3, 256, 64, 1024], P(None, 'gx', 'gy', 'gz'), may hold values from 0.5 to 2
Outputs:
- viscosity: float32 [256, 64, 1024], P('gx', 'gy', 'gz')
- coefficient: float32 [256, 64], P('gx', 'gy')
The draws below stay inside these ranges and needn't reach their ends.
All inputs are finite; a program needn't handle non-finite values.
Results may differ from the reference program's by a relative error of at most 0.0003.
Values sent between devices are 32-bit elements; how exact they have to be, the bound alone decides.
A program may use at most 64 MiB of HBM per device.

```python
import math
import jax
import jax.numpy as jnp
from jax import lax

NX = 256
NY = 64
NZ = 1024


def draw_velocity(key, part):
    noise_key = jax.random.fold_in(key, 11)
    amplitude = 1.0 + 2.0 * jnp.arange(NZ, dtype=jnp.float32) / NZ
    random_part = jax.random.truncated_normal(noise_key, -4.0, 4.0, (3, NX, NY, NZ), jnp.float32)
    return random_part * amplitude


def block_scale(stream_key, dims, pieces, smallest, top_value):
    loudness = 1.0
    for dim, shards_of in pieces:
        heights = jax.random.uniform(jax.random.fold_in(jax.random.fold_in(stream_key, 6), dim), (shards_of,), jnp.float32, smallest / len(pieces), top_value / len(pieces))
        loudness = loudness * jnp.repeat(jnp.exp(heights), dims[dim] // shards_of).reshape((-1,) + (1,) * (len(dims) - 1 - dim))
    return loudness


def setup_inputs(seed: int = 0) -> dict:
    keys = jax.random.split(jax.random.key(seed), 3)
    return {
        "velocity": draw_velocity(jax.random.fold_in(keys[2], 71), 0),
        "metric": jnp.clip(jnp.exp(math.log(2.0) - 1.3862944 * jax.random.uniform(keys[1], (3, NX, NY, NZ), jnp.float32) ** block_scale(keys[1], (3, NX, NY, NZ), ((1, 16), (2, 4), (3, 4)), -0.2, 0.2)), 0.5, 2.0),
    }


pair_rows = (0, 1, 2, 0, 0, 1)
pair_cols = (0, 1, 2, 1, 2, 2)
pair_weight = (1.0, 1.0, 1.0, 2.0, 2.0, 2.0)
eps_line = 1e-06
ratio_square = 4.0

def pad_axis(values, axis_pos, periodic):
    length_axis = values.shape[axis_pos]
    if periodic:
        return jnp.concatenate([lax.slice_in_dim(values, length_axis - 1, length_axis, axis=axis_pos), values, lax.slice_in_dim(values, 0, 1, axis=axis_pos)], axis=axis_pos)
    widths = [(0, 0)] * values.ndim
    widths[axis_pos] = (1, 1)
    return jnp.pad(values, widths)

def box_three(padded, axis_pos):
    length_axis = padded.shape[axis_pos]
    lower_side = lax.slice_in_dim(padded, 0, length_axis - 2, axis=axis_pos)
    middle = lax.slice_in_dim(padded, 1, length_axis - 1, axis=axis_pos)
    upper_side = lax.slice_in_dim(padded, 2, length_axis, axis=axis_pos)
    return 0.25 * lower_side + 0.5 * middle + 0.25 * upper_side

def gradient_field(velocity_part, metric):
    columns = []
    for direction in range(3):
        padded = pad_axis(velocity_part, direction + 1, direction == 2)
        length_axis = padded.shape[direction + 1]
        differ = lax.slice_in_dim(padded, 2, length_axis, axis=direction + 1) - lax.slice_in_dim(padded, 0, length_axis - 2, axis=direction + 1)
        columns.append(0.5 * metric[direction] * differ)
    return jnp.stack(columns, axis=1)

def strain_parts(gradients):
    strain = 0.5 * (gradients + jnp.swapaxes(gradients, 0, 1))
    magnitude = jnp.sqrt(2.0 * lax.optimization_barrier(jnp.sum(strain * strain, axis=(0, 1))))
    strain_pairs = jnp.stack([strain[row_index, col_index] for row_index, col_index in zip(pair_rows, pair_cols)])
    return (strain_pairs, magnitude)

def make_fields(velocity_part, strain_pairs, magnitude):
    products = jnp.stack([velocity_part[row_index] * velocity_part[col_index] for row_index, col_index in zip(pair_rows, pair_cols)])
    return jnp.concatenate([velocity_part, products, magnitude[None] * strain_pairs], axis=0)

def germano(filtered, strain_hat, magnitude_hat, delta_sq):
    numerator = jnp.zeros_like(delta_sq)
    denominator = jnp.zeros_like(delta_sq)
    for position in range(6):
        row_index = pair_rows[position]
        col_index = pair_cols[position]
        leonard = filtered[3 + position] - filtered[row_index] * filtered[col_index]
        model_term = 2.0 * delta_sq * (filtered[9 + position] - ratio_square * magnitude_hat * strain_hat[position])
        numerator = numerator + pair_weight[position] * leonard * model_term
        denominator = denominator + pair_weight[position] * model_term * model_term
    return (numerator, denominator)

def reference(velocity, metric):
    delta_sq = (metric[0] * metric[1] * metric[2]) ** (-2.0 / 3.0)
    strain_pairs, magnitude = strain_parts(gradient_field(velocity, metric))
    fields = make_fields(velocity, strain_pairs, magnitude)
    filtered = box_three(pad_axis(fields, 1, False), 1)
    filtered = box_three(pad_axis(filtered, 2, False), 2)
    filtered = box_three(pad_axis(filtered, 3, True), 3)
    strain_hat, magnitude_hat = strain_parts(gradient_field(filtered[0:3], metric))
    numerator, denominator = germano(filtered, strain_hat, magnitude_hat, delta_sq)
    line_num = lax.optimization_barrier(jnp.sum(numerator, axis=2)) / NZ
    line_den = lax.optimization_barrier(jnp.sum(denominator, axis=2)) / NZ
    line_coef = line_num / (line_den + eps_line)
    peak_coef = jnp.max(line_coef)
    coefficient = jnp.minimum(line_coef, 0.5 * peak_coef)
    viscosity = coefficient[:, :, None] * delta_sq * magnitude
    return (viscosity, coefficient)
```

```python
import functools
import jax
import jax.numpy as jnp
from jax import lax
from jax.experimental import pallas as pl
from jax.experimental.pallas import tpu as pltpu
from jax.sharding import PartitionSpec as P

PAIRS = ((0, 0), (1, 1), (2, 2), (0, 1), (0, 2), (1, 2))
F32 = jnp.float32
MESH = pl.DeviceIdType.MESH
PITCH = 32
BASE = 8


def strain_of(diffs, m):
    g = [[m[j] * diffs[i][j] for j in range(3)] for i in range(3)]
    s = [g[a][a] if a == b else g[a][b] + g[b][a] for a, b in PAIRS]
    diag = s[0] * s[0] + s[1] * s[1] + s[2] * s[2]
    off = s[3] * s[3] + s[4] * s[4] + s[5] * s[5]
    return s, jnp.sqrt(0.5 * diag + 0.25 * off)


def kernel(sizes, vel, met, visc, coef_out, U, O6, SY, RY, SC, RC, RO, ZG, SZX, RZX, SZY, RZY,
           RZC, TZ, UE, ZE, VE, VHE, T, YF, YV, VH, MB, DM, LN, RX, RZ, PK, lsem, ssem, rsem):
    ngx, ngy, ngz = sizes
    nx = vel.shape[1]
    ny = vel.shape[2]
    nz = vel.shape[3]
    gx, gy, gz = lax.axis_index("gx"), lax.axis_index("gy"), lax.axis_index("gz")
    nzc = ngx // 2
    xlo, xz = lax.rem(gx, 2), lax.div(gx, 2)
    has = {("x", 0): gx > 0, ("x", 1): gx < ngx - 1, ("y", 0): gy > 0, ("y", 1): gy < ngy - 1}

    ins = []
    for zt in range(2):
        for k, ref in enumerate((vel, met)):
            cp = pltpu.make_async_copy(
                ref.at[:, :, :, pl.ds(128 * zt, 128)],
                U.at[pl.ds(3 * k, 3), zt, pl.ds(2, nx), pl.ds(BASE, ny), :],
                lsem.at[2 * zt + k],
            )
            cp.start()
            ins.append(cp)

    z8 = jnp.zeros((8, 128), F32)
    for f in range(6):
        for zt in range(2):
            for X in (0, 1, nx + 2, nx + 3):
                for r in range(0, ny, 8):
                    U[f, zt, X, BASE + r : BASE + r + 8, :] = z8
    RY[...] = jnp.zeros(RY.shape, F32)
    RC[...] = jnp.zeros(RC.shape, F32)
    RZX[...] = jnp.zeros(RZX.shape, F32)
    RZY[...] = jnp.zeros(RZY.shape, F32)
    RZC[...] = jnp.zeros(RZC.shape, F32)

    bar = pltpu.get_barrier_semaphore()

    def greet(dev):
        pl.semaphore_signal(bar, inc=1, device_id=dev, device_id_type=MESH)

    def dx(s):
        return gx + (1 if s else -1)

    def dy(s):
        return gy + (1 if s else -1)

    for k in range(1, ngz):
        greet({"gz": lax.rem(gz + k, ngz)})
    for s in range(2):
        @pl.when(has["x", s])
        def _():
            greet({"gx": dx(s)})

        @pl.when(has["y", s])
        def _():
            greet({"gy": dy(s)})

        for q in range(2):
            @pl.when(jnp.logical_and(has["x", s], has["y", q]))
            def _():
                greet({"gx": dx(s), "gy": dy(q)})

    nxc = 2 * ngy
    me_c = xlo * ngy + gy

    def xc_dev(k):
        c = lax.rem(me_c + k, nxc)
        return c, {"gx": xz * 2 + lax.div(c, ngy), "gy": lax.rem(c, ngy)}

    def z_dev(k):
        c = lax.rem(xz + k, nzc)
        return c, {"gx": c * 2 + xlo}

    for k in range(1, nxc):
        greet(xc_dev(k)[1])
    for k in range(1, nzc):
        greet(z_dev(k)[1])
    ex = has["x", 0].astype(jnp.int32) + has["x", 1].astype(jnp.int32)
    ey = has["y", 0].astype(jnp.int32) + has["y", 1].astype(jnp.int32)

    lane = lax.broadcasted_iota(jnp.int32, (8, 128), 1)
    lx = lax.shift_right_logical(lane * 43, 8)
    lc = lane - 6 * lx
    row = lax.broadcasted_iota(jnp.int32, (8, 128), 0)
    for cp in ins:
        cp.wait()
    half = lane < 64
    for f in range(6):
        for t in range(2):
            acc = z8
            rows = slice(BASE + 8 * t, BASE + 8 * t + 8)
            for X in range(2, nx + 2):
                a = jnp.where(half, U[f, 0, X, rows, :], U[f, 1, X, rows, :])
                acc = jnp.where(lx == X, pltpu.roll(a, (6 * X + 2) % 128, 1), acc)
            O6[f, 8 * t : 8 * t + 8, :] = acc

    for s in range(2):
        for f in range(6):
            for k in range(2):
                if f >= 3 and k != s:
                    continue
                y = (ny - 2 + k) if s else k
                slab = 2 * f + k if f < 3 else 3 + f
                for zt in range(2):
                    SY[s, slab, zt, :, :] = U[f, zt, pl.ds(2, nx), BASE + y, :]

    def corner_rows(out, sx, sy):
        r = 0
        for f in range(6):
            for kx in range(2):
                for ky in range(2):
                    if f >= 3 and (kx != sx or ky != sy):
                        continue
                    if out:
                        X = (nx if sx else 2) + kx
                        y = (ny - 2 if sy else 0) + ky
                    else:
                        X = (nx + 2 if sx else 0) + kx
                        y = (ny if sy else -2) + ky
                    yield r, f, X, y + BASE
                    r += 1

    for sx in range(2):
        for sy in range(2):
            for r, f, X, yr in corner_rows(True, sx, sy):
                for zt in range(2):
                    SC[2 * sx + sy, zt, r : r + 1, :] = U[f, zt, X, yr : yr + 1, :]

    pl.semaphore_wait(bar, (ngz - 1) + (nxc - 1) + (nzc - 1) + ex + ey + ex * ey)

    waits_send, waits_recv = [], {}

    def put(n, src, dst, dev, send_if=None, recv_if=None):
        cp = pltpu.make_async_remote_copy(
            src_ref=src, dst_ref=dst, send_sem=ssem.at[n], recv_sem=rsem.at[n],
            device_id=dev, device_id_type=MESH)
        if send_if is None:
            cp.start()
        else:
            pl.when(send_if)(cp.start)
        waits_send.append((cp, send_if))
        waits_recv[n] = (cp, recv_if)

    def got(n):
        cp, cond = waits_recv[n]
        if cond is None:
            cp.wait_recv()
        else:
            pl.when(cond)(cp.wait_recv)

    for s in range(2):
        put(s, O6, RO.at[1 - s], {"gz": lax.rem(gz + (1 if s else ngz - 1), ngz)})
    for s in range(2):
        put(2 + s, SY.at[s], RY.at[1 - s], {"gy": dy(s)}, has["y", s], has["y", 1 - s])
    for sx in range(2):
        for sy in range(2):
            c, o = 2 * sx + sy, 2 * (1 - sx) + 1 - sy
            put(8 + c, SC.at[c], RC.at[o], {"gx": dx(sx), "gy": dy(sy)},
                jnp.logical_and(has["x", sx], has["y", sy]),
                jnp.logical_and(has["x", 1 - sx], has["y", 1 - sy]))
    rr = pl.ds(BASE, ny)
    for s in range(2):
        far, near = (nx, nx + 1) if s else (3, 2)
        gfar, gnear = (0, 1) if s else (nx + 3, nx + 2)
        put(4 + s, U.at[:, :, near, rr, :], U.at[:, :, gnear, rr, :], {"gx": dx(s)},
            has["x", s], has["x", 1 - s])
        put(6 + s, U.at[pl.ds(0, 3), :, far, rr, :], U.at[pl.ds(0, 3), :, gfar, rr, :],
            {"gx": dx(s)}, has["x", s], has["x", 1 - s])

    got(0)
    got(1)
    lanes_x = jnp.logical_and(lx >= 2, lx < nx + 2)
    for f in range(6):
        ZG[f, 0:8, :] = z8
        ZG[f, 24:32, :] = z8
        for t in range(2):
            rows = slice(8 * t, 8 * t + 8)
            own = O6[f, rows, :]
            right = pltpu.roll(jnp.where(lc == 1, own, RO[1, f, rows, :]), 2, 1)
            z = jnp.where(lc < 2, RO[0, f, rows, :], jnp.where(lc == 2, own, right))
            ZG[f, BASE + 8 * t : BASE + 8 * t + 8, :] = jnp.where(lanes_x, z, 0.0)
    for s in range(2):
        first = 6 * (nx if s else 2)
        for t in range(2):
            acc = z8
            for f in range(6):
                part = pltpu.roll(ZG[f, BASE + 8 * t : BASE + 8 * t + 8, :], (12 * f - first) % 128, 1)
                acc = jnp.where(jnp.logical_and(lane >= 12 * f, lane < 12 * f + 12), part, acc)
            SZX[s, 8 * t : 8 * t + 8, :] = acc
        y = ny - 2 if s else 0
        for f in range(6):
            SZY[s, 2 * f : 2 * f + 2, :] = ZG[f, BASE + y : BASE + y + 2, :]
    for s in range(2):
        put(14 + s, SZY.at[s], RZY.at[1 - s], {"gy": dy(s)}, has["y", s], has["y", 1 - s])
        put(12 + s, SZX.at[s], RZX.at[1 - s], {"gx": dx(s)}, has["x", s], has["x", 1 - s])
    for sx in range(2):
        for sy in range(2):
            c, o = 2 * sx + sy, 2 * (1 - sx) + 1 - sy
            put(16 + c, SZX.at[sx, pl.ds(ny - 8 if sy else 0, 8), :], RZC.at[o],
                {"gx": dx(sx), "gy": dy(sy)},
                jnp.logical_and(has["x", sx], has["y", sy]),
                jnp.logical_and(has["x", 1 - sx], has["y", 1 - sy]))

    for n in range(2, 20):
        got(n)

    for s in range(2):
        for f in range(6):
            for k in range(2):
                if f >= 3 and k == s:
                    continue
                y = (ny + k) if s else k - 2
                slab = 2 * f + k if f < 3 else 3 + f
                for zt in range(2):
                    U[f, zt, pl.ds(2, nx), BASE + y, :] = RY[s, slab, zt, :, :]
    for sx in range(2):
        for sy in range(2):
            src = {}
            r = 0
            for f in range(6):
                for kx in range(2):
                    for ky in range(2):
                        if f >= 3 and (kx != 1 - sx or ky != 1 - sy):
                            continue
                        src[f, kx, ky] = r
                        r += 1
            for (f, kx, ky), r in src.items():
                X = (nx + 2 if sx else 0) + kx
                yr = (ny if sy else -2) + ky + BASE
                for zt in range(2):
                    U[f, zt, X, yr : yr + 1, :] = RC[2 * sx + sy, zt, r : r + 1, :]
    for f in range(6):
        for t in range(2):
            rows = slice(BASE + 8 * t, BASE + 8 * t + 8)
            z = ZG[f, rows, :]
            for s in range(2):
                at = 6 * (nx + 2) if s else 0
                part = pltpu.roll(RZX[s, 8 * t : 8 * t + 8, :], (at - 12 * f) % 128, 1)
                z = jnp.where(jnp.logical_and(lane >= at, lane < at + 12), part, z)
            ZG[f, rows, :] = z
        for sy in range(2):
            yr = BASE + (ny if sy else -2)
            z = RZY[sy, 2 * f : 2 * f + 2, :]
            for sx in range(2):
                at = 6 * (nx + 2) if sx else 0
                tile = RZC[2 * sx + sy]
                part = pltpu.roll(tile, (at - 12 * f) % 128, 1)
                part = part[0:2] if sy else part[6:8]
                lane2 = lane[0:2]
                z = jnp.where(jnp.logical_and(lane2 >= at, lane2 < at + 12), part, z)
            ZG[f, yr : yr + 2, :] = z

    def edge(a):
        return jnp.where(lc == 0, pltpu.roll(a, 124, 1), a)

    def xsum(a):
        return pltpu.roll(a, 6, 1) + 2.0 * a + pltpu.roll(a, 122, 1)

    xd = lambda a: pltpu.roll(a, 122, 1) - pltpu.roll(a, 6, 1)
    zd = lambda a: pltpu.roll(a, 127, 1) - pltpu.roll(a, 1, 1)
    for t in range(3):
        r0 = BASE - 1 + 8 * t
        at = lambda f, d: ZG[f, r0 + d : r0 + d + 8, :]
        u = [at(i, 0) for i in range(3)]
        up = [at(i, 1) for i in range(3)]
        dn = [at(i, -1) for i in range(3)]
        m = [at(3 + j, 0) for j in range(3)]
        d = [[xd(u[i]), up[i] - dn[i], zd(u[i])] for i in range(3)]
        s, mag = strain_of(d, m)
        for p, (a, b) in enumerate(PAIRS):
            TZ[p, 8 * t : 8 * t + 8, :] = u[a] * u[b]
            TZ[6 + p, 8 * t : 8 * t + 8, :] = (0.5 if a == b else 0.25) * mag * s[p]
        for i in range(3):
            UE[i, 8 * t : 8 * t + 8, :] = edge(u[i])
            v = xsum(up[i] + dn[i] + 2.0 * u[i])
            VE[i, 8 * t : 8 * t + 8, :] = edge(v)
            vz = (1.0 / 64.0) * (pltpu.roll(v, 1, 1) + 2.0 * v + pltpu.roll(v, 127, 1))
            VHE[i, 8 * t : 8 * t + 8, :] = edge(vz)
    for p in range(12):
        for t in range(2):
            a = TZ[p, 8 * t : 8 * t + 8, :] + 2.0 * TZ[p, 8 * t + 1 : 8 * t + 9, :] + TZ[p, 8 * t + 2 : 8 * t + 10, :]
            ZE[p, 8 * t : 8 * t + 8, :] = edge(xsum(a))

    first_lane, last_lane = lane == 0, lane == 127

    def zshift(a, e):
        p0, p1 = pltpu.roll(a[0], 1, 1), pltpu.roll(a[1], 1, 1)
        n0, n1 = pltpu.roll(a[0], 127, 1), pltpu.roll(a[1], 127, 1)
        prev = (jnp.where(first_lane, e, p0), jnp.where(first_lane, p0, p1))
        nxt = (jnp.where(last_lane, n1, n0), jnp.where(last_lane, e, n1))
        return prev, nxt

    def stage_a(X, _):
        turn = 127 - 6 * X
        for t in range(3):
            r0 = BASE - 1 + 8 * t
            u = [[U[i, zt, X, r0 : r0 + 8, :] for zt in range(2)] for i in range(3)]
            zs = [zshift(u[i], pltpu.roll(UE[i, 8 * t : 8 * t + 8, :], turn, 1)) for i in range(3)]
            for zt in range(2):
                d = []
                for i in range(3):
                    ddx = U[i, zt, X + 1, r0 : r0 + 8, :] - U[i, zt, X - 1, r0 : r0 + 8, :]
                    ddy = U[i, zt, X, r0 + 1 : r0 + 9, :] - U[i, zt, X, r0 - 1 : r0 + 7, :]
                    d.append([ddx, ddy, zs[i][1][zt] - zs[i][0][zt]])
                m = [U[3 + j, zt, X, r0 : r0 + 8, :] for j in range(3)]
                s, mag = strain_of(d, m)
                for p, (a, b) in enumerate(PAIRS):
                    T[p, zt, 8 * t : 8 * t + 8, :] = u[a][zt] * u[b][zt]
                    T[6 + p, zt, 8 * t : 8 * t + 8, :] = (0.5 if a == b else 0.25) * mag * s[p]
                MB[X, zt, 8 * t : 8 * t + 8, :] = mag
        for p in range(12):
            for zt in range(2):
                for t in range(2):
                    r = 8 * t
                    YF[p, zt, X, r : r + 8, :] = (
                        T[p, zt, r : r + 8, :] + 2.0 * T[p, zt, r + 1 : r + 9, :] + T[p, zt, r + 2 : r + 10, :])
        return 0

    lax.fori_loop(1, nx + 3, stage_a, 0)

    def stage_y(X, _):
        for i in range(3):
            for zt in range(2):
                for t in range(3):
                    r = BASE - 1 + 8 * t
                    YV[i, zt, X, 8 * t : 8 * t + 8, :] = (
                        U[i, zt, X, r - 1 : r + 7, :] + 2.0 * U[i, zt, X, r : r + 8, :] + U[i, zt, X, r + 1 : r + 9, :])
        return 0

    lax.fori_loop(0, nx + 4, stage_y, 0)

    def stage_v(X, _):
        turn = 127 - 6 * X
        x_in = jnp.logical_and(jnp.logical_or(X >= 2, gx > 0), jnp.logical_or(X < nx + 2, gx < ngx - 1))
        for t in range(3):
            rr_ = row + 8 * t
            y_in = jnp.logical_and(rr_ >= jnp.where(gy > 0, 0, 1), rr_ < jnp.where(gy < ngy - 1, ny + 2, ny + 1))
            inside = jnp.logical_and(y_in, x_in)
            for i in range(3):
                a = [YV[i, zt, X - 1, 8 * t : 8 * t + 8, :] + 2.0 * YV[i, zt, X, 8 * t : 8 * t + 8, :]
                     + YV[i, zt, X + 1, 8 * t : 8 * t + 8, :] for zt in range(2)]
                prev, nxt = zshift(a, pltpu.roll(VE[i, 8 * t : 8 * t + 8, :], turn, 1))
                for zt in range(2):
                    v = (1.0 / 64.0) * (prev[zt] + 2.0 * a[zt] + nxt[zt])
                    VH[i, zt, X, 8 * t : 8 * t + 8, :] = jnp.where(inside, v, 0.0)
        return 0

    lax.fori_loop(1, nx + 3, stage_v, 0)

    LN[gz] = z8

    def stage_c(X, _):
        turn = 127 - 6 * X
        for t in range(2):
            r = 8 * t
            v = [[VH[i, zt, X, r + 1 : r + 9, :] for zt in range(2)] for i in range(3)]
            zs = [zshift(v[i], pltpu.roll(VHE[i, r + 1 : r + 9, :], turn, 1)) for i in range(3)]
            fl = []
            for p in range(12):
                a = [YF[p, zt, X - 1, r : r + 8, :] + 2.0 * YF[p, zt, X, r : r + 8, :]
                     + YF[p, zt, X + 1, r : r + 8, :] for zt in range(2)]
                prev, nxt = zshift(a, pltpu.roll(ZE[p, r : r + 8, :], turn, 1))
                fl.append([(1.0 / 64.0) * (prev[zt] + 2.0 * a[zt] + nxt[zt]) for zt in range(2)])
            num = den = None
            for zt in range(2):
                d = []
                for i in range(3):
                    ddx = VH[i, zt, X + 1, r + 1 : r + 9, :] - VH[i, zt, X - 1, r + 1 : r + 9, :]
                    ddy = VH[i, zt, X, r + 2 : r + 10, :] - VH[i, zt, X, r : r + 8, :]
                    d.append([ddx, ddy, zs[i][1][zt] - zs[i][0][zt]])
                m = [U[3 + j, zt, X, BASE + r : BASE + r + 8, :] for j in range(3)]
                s, mag = strain_of(d, m)
                delta = jnp.exp2((-2.0 / 3.0) * jnp.log2(m[0] * m[1] * m[2]))
                nn = dd = None
                for p, (a, b) in enumerate(PAIRS):
                    w = 1.0 if a == b else 2.0
                    leo = fl[p][zt] - v[a][zt] * v[b][zt]
                    q = fl[6 + p][zt] - (2.0 if a == b else 1.0) * mag * s[p]
                    wq = q if a == b else w * q
                    n_, d_ = wq * leo, wq * q
                    nn = n_ if nn is None else nn + n_
                    dd = d_ if dd is None else dd + d_
                d2 = 2.0 * delta
                n_, d_ = d2 * nn, d2 * d2 * dd
                num = n_ if num is None else num + n_
                den = d_ if den is None else den + d_
                DM[X - 2, zt, r : r + 8, :] = delta * MB[X, zt, r + 1 : r + 9, :]
            at = X - 2 + nx * t
            ln = jnp.where(lane == at, jnp.sum(num, axis=1, keepdims=True), LN[gz])
            LN[gz] = jnp.where(lane == at + 2 * nx, jnp.sum(den, axis=1, keepdims=True), ln)
        return 0

    lax.fori_loop(2, nx + 2, stage_c, 0)

    cps = []
    for k in range(1, ngz):
        cp = pltpu.make_async_remote_copy(
            src_ref=LN.at[gz], dst_ref=LN.at[gz], send_sem=ssem.at[20 + k], recv_sem=rsem.at[20 + gz],
            device_id={"gz": lax.rem(gz + k, ngz)}, device_id_type=MESH)
        cp.start()
        cps.append(cp)
    for k in range(1, ngz):
        src = lax.rem(gz + k, ngz)
        pltpu.make_async_remote_copy(
            src_ref=LN.at[gz], dst_ref=LN.at[src], send_sem=ssem.at[20 + k], recv_sem=rsem.at[20 + src],
            device_id={"gz": src}, device_id_type=MESH).wait_recv()
    tot = LN[0]
    for k in range(1, ngz):
        tot = tot + LN[k]
    tot = tot * (1.0 / (nz * ngz))
    den = pltpu.roll(tot, 128 - 2 * nx, 1)
    line = tot / (den + 1e-06)
    valid = lane < 2 * nx
    peak = jnp.max(jnp.where(valid, line, -jnp.inf), axis=0, keepdims=True)
    peak = jnp.max(peak, axis=1, keepdims=True)

    RX[me_c] = jnp.broadcast_to(peak, (1, 128))
    for k in range(1, nxc):
        c, dev = xc_dev(k)
        cp = pltpu.make_async_remote_copy(
            src_ref=RX.at[me_c], dst_ref=RX.at[me_c], send_sem=ssem.at[24 + k], recv_sem=rsem.at[24 + me_c],
            device_id=dev, device_id_type=MESH)
        cp.start()
        cps.append(cp)
    for k in range(1, nxc):
        c, dev = xc_dev(k)
        pltpu.make_async_remote_copy(
            src_ref=RX.at[me_c], dst_ref=RX.at[c], send_sem=ssem.at[24 + k], recv_sem=rsem.at[24 + c],
            device_id=dev, device_id_type=MESH).wait_recv()
    peak = RX[0]
    for k in range(1, nxc):
        peak = jnp.maximum(peak, RX[k])
    RZ[xz] = peak
    for k in range(1, nzc):
        c, dev = z_dev(k)
        cp = pltpu.make_async_remote_copy(
            src_ref=RZ.at[xz], dst_ref=RZ.at[xz], send_sem=ssem.at[32 + k], recv_sem=rsem.at[32 + xz],
            device_id=dev, device_id_type=MESH)
        cp.start()
        cps.append(cp)
    for k in range(1, nzc):
        c, dev = z_dev(k)
        pltpu.make_async_remote_copy(
            src_ref=RZ.at[xz], dst_ref=RZ.at[c], send_sem=ssem.at[32 + k], recv_sem=rsem.at[32 + c],
            device_id=dev, device_id_type=MESH).wait_recv()
    peak = RZ[0]
    for k in range(1, nzc):
        peak = jnp.maximum(peak, RZ[k])

    coef = jnp.minimum(line, 0.5 * peak)
    for x in range(nx):
        for t in range(2):
            at = x + nx * t
            cb = jnp.broadcast_to(coef[:, at : at + 1], (8, 128))
            for zt in range(2):
                visc[x, 8 * t : 8 * t + 8, 128 * zt : 128 * zt + 128] = cb * DM[x, zt, 8 * t : 8 * t + 8, :]
    ct = coef.T
    for t in range(2):
        coef_out[:, 8 * t : 8 * t + 8] = ct[nx * t : nx * t + nx, :]

    for cp in cps:
        cp.wait_send()
    for cp, cond in waits_send:
        if cond is None:
            cp.wait_send()
        else:
            pl.when(cond)(cp.wait_send)


def solution(mesh):
    sizes = tuple(mesh.shape[a] for a in ("gx", "gy", "gz"))
    ngx, ngy, ngz = sizes

    def per_device(velocity, metric):
        _, nx, ny, nz = velocity.shape
        vm = lambda *s: pltpu.VMEM(s, F32)
        return pl.pallas_call(
            functools.partial(kernel, sizes),
            out_shape=(jax.ShapeDtypeStruct((nx, ny, nz), F32), jax.ShapeDtypeStruct((nx, ny), F32)),
            in_specs=[pl.BlockSpec(memory_space=pl.ANY)] * 2,
            out_specs=(pl.BlockSpec(memory_space=pltpu.VMEM),) * 2,
            scratch_shapes=[
                vm(6, 2, nx + 4, PITCH, 128),
                vm(6, 16, 128),
                vm(2, 9, 2, nx, 128),
                vm(2, 9, 2, nx, 128),
                vm(4, 2, 16, 128),
                vm(4, 2, 16, 128),
                vm(2, 6, 16, 128),
                vm(6, 32, 128),
                vm(2, 16, 128),
                vm(2, 16, 128),
                vm(2, 16, 128),
                vm(2, 16, 128),
                vm(4, 8, 128),
                vm(12, 24, 128),
                vm(3, 24, 128),
                vm(12, 16, 128),
                vm(3, 24, 128),
                vm(3, 24, 128),
                vm(12, 2, 24, 128),
                vm(12, 2, nx + 4, 16, 128),
                vm(3, 2, nx + 4, 24, 128),
                vm(3, 2, nx + 4, 24, 128),
                vm(nx + 4, 2, 24, 128),
                vm(nx, 2, 16, 128),
                vm(ngz, 8, 128),
                vm(2 * ngy, 1, 128),
                vm(ngx // 2, 1, 128),
                vm(1, 128),
                pltpu.SemaphoreType.DMA((4,)),
                pltpu.SemaphoreType.DMA((40,)),
                pltpu.SemaphoreType.DMA((40,)),
            ],
            compiler_params=pltpu.CompilerParams(collective_id=0, has_side_effects=True),
        )(velocity, metric)

    return jax.shard_map(
        per_device,
        mesh=mesh,
        in_specs=(P(None, "gx", "gy", "gz"), P(None, "gx", "gy", "gz")),
        out_specs=(P("gx", "gy", "gz"), P("gx", "gy")),
        check_vma=False,
    )
```

```python
import functools
import jax
import jax.numpy as jnp
from jax import lax
from jax.experimental import pallas as pl
from jax.experimental.pallas import tpu as pltpu
from jax.sharding import PartitionSpec as P

PAIRS = ((0, 0), (1, 1), (2, 2), (0, 1), (0, 2), (1, 2))
F32 = jnp.float32
MESH = pl.DeviceIdType.MESH
PITCH = 32
BASE = 8


def strain_of(diffs, m):
    g = [[m[j] * diffs[i][j] for j in range(3)] for i in range(3)]
    s = [g[a][a] if a == b else g[a][b] + g[b][a] for a, b in PAIRS]
    diag = s[0] * s[0] + s[1] * s[1] + s[2] * s[2]
    off = s[3] * s[3] + s[4] * s[4] + s[5] * s[5]
    return s, jnp.sqrt(0.5 * diag + 0.25 * off)


def kernel(sizes, vel, met, dm_out, line_out, half_out, U, O6, SY, RY, SC, RC, RO, ZG, SZX, RZX, SZY, RZY,
           RZC, SZG, TZ, UE, ZE, VE, VHE, T, YF, YV, VH, MB, DM, LN, RX, RZ, lsem, ssem, rsem):
    ngx, ngy, ngz = sizes
    nx = vel.shape[1]
    ny = vel.shape[2]
    nz = vel.shape[3]
    gx, gy, gz = lax.axis_index("gx"), lax.axis_index("gy"), lax.axis_index("gz")
    nzc = ngx // 2
    xlo, xz = lax.rem(gx, 2), lax.div(gx, 2)
    has = {("x", 0): gx > 0, ("x", 1): gx < ngx - 1, ("y", 0): gy > 0, ("y", 1): gy < ngy - 1}

    ins = []
    for zt in range(2):
        for k, ref in enumerate((vel, met)):
            cp = pltpu.make_async_copy(
                ref.at[:, :, :, pl.ds(128 * zt, 128)],
                U.at[pl.ds(3 * k, 3), zt, pl.ds(2, nx), pl.ds(BASE, ny), :],
                lsem.at[2 * zt + k],
            )
            cp.start()
            ins.append(cp)

    bar = pltpu.get_barrier_semaphore()

    def greet(dev):
        pl.semaphore_signal(bar, inc=1, device_id=dev, device_id_type=MESH)

    def dx(s):
        return gx + (1 if s else -1)

    def dy(s):
        return gy + (1 if s else -1)

    def gz_at(d):
        return lax.rem(gz + d + ngz, ngz)

    both = {(sx, sy): jnp.logical_and(has["x", sx], has["y", sy]) for sx in range(2) for sy in range(2)}
    for d in (-1, 1):
        greet({"gz": gz_at(d)})
    for s in range(2):
        @pl.when(has["y", s])
        def _():
            for d in (-1, 0, 1):
                greet({"gy": dy(s), "gz": gz_at(d)})

        @pl.when(has["x", s])
        def _():
            for d in (-1, 0, 1):
                greet({"gx": dx(s), "gz": gz_at(d)})

        for q in range(2):
            @pl.when(both[s, q])
            def _():
                for d in (-1, 0, 1):
                    greet({"gx": dx(s), "gy": dy(q), "gz": gz_at(d)})

    for k in range(2, ngz - 1):
        greet({"gz": gz_at(k)})

    nxc = 2 * ngy
    me_c = xlo * ngy + gy

    def xc_dev(k):
        c = lax.rem(me_c + k, nxc)
        return c, {"gx": xz * 2 + lax.div(c, ngy), "gy": lax.rem(c, ngy)}

    def z_dev(k):
        c = lax.rem(xz + k, nzc)
        return c, {"gx": c * 2 + xlo}

    for k in range(1, nxc):
        greet(xc_dev(k)[1])
    for k in range(1, nzc):
        greet(z_dev(k)[1])
    ex = has["x", 0].astype(jnp.int32) + has["x", 1].astype(jnp.int32)
    ey = has["y", 0].astype(jnp.int32) + has["y", 1].astype(jnp.int32)
    partners = 3 * (1 + ex) * (1 + ey) - 1 + max(ngz - 3, 0) + (nxc - 1) + (nzc - 1)

    z8 = jnp.zeros((8, 128), F32)
    for s in range(2):
        @pl.when(jnp.logical_not(has["x", s]))
        def _():
            for f in range(6):
                for zt in range(2):
                    for X in ((nx + 2, nx + 3) if s else (0, 1)):
                        for r in range(0, ny, 8):
                            U[f, zt, X, BASE + r : BASE + r + 8, :] = z8
            for d in range(3):
                RZX[d, s] = jnp.zeros(RZX.shape[2:], F32)

        @pl.when(jnp.logical_not(has["y", s]))
        def _():
            RY[s] = jnp.zeros(RY.shape[1:], F32)
            for d in range(3):
                RZY[d, s] = jnp.zeros(RZY.shape[2:], F32)

        for q in range(2):
            @pl.when(jnp.logical_not(both[s, q]))
            def _():
                RC[2 * s + q] = jnp.zeros(RC.shape[1:], F32)
                for d in range(3):
                    RZC[d, 2 * s + q] = z8

    lane = lax.broadcasted_iota(jnp.int32, (8, 128), 1)
    lx = lax.shift_right_logical(lane * 43, 8)
    lc = lane - 6 * lx
    row = lax.broadcasted_iota(jnp.int32, (8, 128), 0)
    for cp in ins:
        cp.wait()
    half = lane < 64
    for f in range(6):
        for t in range(2):
            acc = z8
            rows = slice(BASE + 8 * t, BASE + 8 * t + 8)
            for X in range(2, nx + 2):
                a = jnp.where(half, U[f, 0, X, rows, :], U[f, 1, X, rows, :])
                acc = jnp.where(lx == X, pltpu.roll(a, (6 * X + 2) % 128, 1), acc)
            O6[f, 8 * t : 8 * t + 8, :] = acc

    for s in range(2):
        first = 6 * (nx if s else 2)
        for t in range(2):
            acc = z8
            for f in range(6):
                part = pltpu.roll(O6[f, 8 * t : 8 * t + 8, :], (12 * f - first) % 128, 1)
                acc = jnp.where(jnp.logical_and(lane >= 12 * f, lane < 12 * f + 12), part, acc)
            SZX[s, 8 * t : 8 * t + 8, :] = acc
        y = ny - 2 if s else 0
        for f in range(6):
            SZY[s, 2 * f : 2 * f + 2, :] = O6[f, y : y + 2, :]
        SZY[s, 12:16, :] = z8[0:4]

    for s in range(2):
        for f in range(6):
            for k in range(2):
                if f >= 3 and k != s:
                    continue
                y = (ny - 2 + k) if s else k
                slab = 2 * f + k if f < 3 else 3 + f
                for zt in range(2):
                    SY[s, slab, zt, :, :] = U[f, zt, pl.ds(2, nx), BASE + y, :]

    def corner_rows(out, sx, sy):
        r = 0
        for f in range(6):
            for kx in range(2):
                for ky in range(2):
                    if f >= 3 and (kx != sx or ky != sy):
                        continue
                    if out:
                        X = (nx if sx else 2) + kx
                        y = (ny - 2 if sy else 0) + ky
                    else:
                        X = (nx + 2 if sx else 0) + kx
                        y = (ny if sy else -2) + ky
                    yield r, f, X, y + BASE
                    r += 1

    for sx in range(2):
        for sy in range(2):
            for r, f, X, yr in corner_rows(True, sx, sy):
                for zt in range(2):
                    SC[2 * sx + sy, zt, r : r + 1, :] = U[f, zt, X, yr : yr + 1, :]

    pl.semaphore_wait(bar, partners)

    waits_send, waits_recv = [], {}

    def put(n, src, dst, dev, send_if=None, recv_if=None):
        cp = pltpu.make_async_remote_copy(
            src_ref=src, dst_ref=dst, send_sem=ssem.at[n], recv_sem=rsem.at[n],
            device_id=dev, device_id_type=MESH)
        if send_if is None:
            cp.start()
        else:
            pl.when(send_if)(cp.start)
        waits_send.append((cp, send_if))
        waits_recv[n] = (cp, recv_if)

    def got(n):
        cp, cond = waits_recv[n]
        if cond is None:
            cp.wait_recv()
        else:
            pl.when(cond)(cp.wait_recv)

    for s in range(2):
        put(s, O6, RO.at[1 - s], {"gz": gz_at(1 if s else -1)})
    for i, d in enumerate((-1, 0, 1)):
        o = 2 - i
        for s in range(2):
            put(12 + 2 * i + s, SZY.at[s], RZY.at[o, 1 - s], {"gy": dy(s), "gz": gz_at(d)},
                has["y", s], has["y", 1 - s])
            put(18 + 2 * i + s, SZX.at[s], RZX.at[o, 1 - s], {"gx": dx(s), "gz": gz_at(d)},
                has["x", s], has["x", 1 - s])
        for sx in range(2):
            for sy in range(2):
                put(24 + 4 * i + 2 * sx + sy, SZX.at[sx, pl.ds(ny - 8 if sy else 0, 8), :],
                    RZC.at[o, 2 * (1 - sx) + 1 - sy],
                    {"gx": dx(sx), "gy": dy(sy), "gz": gz_at(d)},
                    both[sx, sy], both[1 - sx, 1 - sy])
    for s in range(2):
        put(2 + s, SY.at[s], RY.at[1 - s], {"gy": dy(s)}, has["y", s], has["y", 1 - s])
    rr = pl.ds(BASE, ny)
    for s in range(2):
        far, near = (nx, nx + 1) if s else (3, 2)
        gfar, gnear = (0, 1) if s else (nx + 3, nx + 2)
        put(4 + s, U.at[:, :, near, rr, :], U.at[:, :, gnear, rr, :], {"gx": dx(s)},
            has["x", s], has["x", 1 - s])
        put(6 + s, U.at[pl.ds(0, 3), :, far, rr, :], U.at[pl.ds(0, 3), :, gfar, rr, :],
            {"gx": dx(s)}, has["x", s], has["x", 1 - s])
    for sx in range(2):
        for sy in range(2):
            put(8 + 2 * sx + sy, SC.at[2 * sx + sy], RC.at[2 * (1 - sx) + 1 - sy],
                {"gx": dx(sx), "gy": dy(sy)}, both[sx, sy], both[1 - sx, 1 - sy])

    def comb(left, own, right):
        return jnp.where(lc < 2, left, jnp.where(lc == 2, own, pltpu.roll(jnp.where(lc == 1, own, right), 2, 1)))

    for n in (0, 1, *range(12, 36)):
        got(n)
    zx, zc = {}, {}
    for s in range(2):
        for t in range(2):
            rows = slice(8 * t, 8 * t + 8)
            zx[s, t] = comb(RZX[0, s, rows, :], RZX[1, s, rows, :], RZX[2, s, rows, :])
            SZG[s, rows, :] = comb(RZY[0, s, rows, :], RZY[1, s, rows, :], RZY[2, s, rows, :])
    for c in range(4):
        zc[c] = comb(RZC[0, c], RZC[1, c], RZC[2, c])
    for f in range(6):
        ZG[f, 0:8, :] = z8
        ZG[f, 24:32, :] = z8
        for t in range(2):
            rows = slice(8 * t, 8 * t + 8)
            z = comb(RO[0, f, rows, :], O6[f, rows, :], RO[1, f, rows, :])
            for s in range(2):
                at = 6 * (nx + 2) if s else 0
                part = pltpu.roll(zx[s, t], (at - 12 * f) % 128, 1)
                z = jnp.where(jnp.logical_and(lane >= at, lane < at + 12), part, z)
            ZG[f, BASE + 8 * t : BASE + 8 * t + 8, :] = z
        for sy in range(2):
            yr = BASE + (ny if sy else -2)
            z = SZG[sy, 2 * f : 2 * f + 2, :]
            for sx in range(2):
                at = 6 * (nx + 2) if sx else 0
                part = pltpu.roll(zc[2 * sx + sy], (at - 12 * f) % 128, 1)
                part = part[0:2] if sy else part[6:8]
                lane2 = lane[0:2]
                z = jnp.where(jnp.logical_and(lane2 >= at, lane2 < at + 12), part, z)
            ZG[f, yr : yr + 2, :] = z

    def edge(a):
        return jnp.where(lc == 0, pltpu.roll(a, 124, 1), a)

    def xsum(a):
        return pltpu.roll(a, 6, 1) + 2.0 * a + pltpu.roll(a, 122, 1)

    xd = lambda a: pltpu.roll(a, 122, 1) - pltpu.roll(a, 6, 1)
    zd = lambda a: pltpu.roll(a, 127, 1) - pltpu.roll(a, 1, 1)
    for t in range(3):
        r0 = BASE - 1 + 8 * t
        at = lambda f, d: ZG[f, r0 + d : r0 + d + 8, :]
        u = [at(i, 0) for i in range(3)]
        up = [at(i, 1) for i in range(3)]
        dn = [at(i, -1) for i in range(3)]
        m = [at(3 + j, 0) for j in range(3)]
        d = [[xd(u[i]), up[i] - dn[i], zd(u[i])] for i in range(3)]
        s, mag = strain_of(d, m)
        for p, (a, b) in enumerate(PAIRS):
            TZ[p, 8 * t : 8 * t + 8, :] = u[a] * u[b]
            TZ[6 + p, 8 * t : 8 * t + 8, :] = (0.5 if a == b else 0.25) * mag * s[p]
        for i in range(3):
            UE[i, 8 * t : 8 * t + 8, :] = edge(u[i])
            v = xsum(up[i] + dn[i] + 2.0 * u[i])
            VE[i, 8 * t : 8 * t + 8, :] = edge(v)
            vz = (1.0 / 64.0) * (pltpu.roll(v, 1, 1) + 2.0 * v + pltpu.roll(v, 127, 1))
            VHE[i, 8 * t : 8 * t + 8, :] = edge(vz)
    for p in range(12):
        for t in range(2):
            a = TZ[p, 8 * t : 8 * t + 8, :] + 2.0 * TZ[p, 8 * t + 1 : 8 * t + 9, :] + TZ[p, 8 * t + 2 : 8 * t + 10, :]
            ZE[p, 8 * t : 8 * t + 8, :] = edge(xsum(a))

    first_lane, last_lane = lane == 0, lane == 127

    def zshift(a, e):
        p0, p1 = pltpu.roll(a[0], 1, 1), pltpu.roll(a[1], 1, 1)
        n0, n1 = pltpu.roll(a[0], 127, 1), pltpu.roll(a[1], 127, 1)
        prev = (jnp.where(first_lane, e, p0), jnp.where(first_lane, p0, p1))
        nxt = (jnp.where(last_lane, n1, n0), jnp.where(last_lane, e, n1))
        return prev, nxt

    def stage_a(X, _):
        turn = 127 - 6 * X
        for t in range(3):
            r0 = BASE - 1 + 8 * t
            u = [[U[i, zt, X, r0 : r0 + 8, :] for zt in range(2)] for i in range(3)]
            zs = [zshift(u[i], pltpu.roll(UE[i, 8 * t : 8 * t + 8, :], turn, 1)) for i in range(3)]
            for zt in range(2):
                d = []
                for i in range(3):
                    ddx = U[i, zt, X + 1, r0 : r0 + 8, :] - U[i, zt, X - 1, r0 : r0 + 8, :]
                    ddy = U[i, zt, X, r0 + 1 : r0 + 9, :] - U[i, zt, X, r0 - 1 : r0 + 7, :]
                    d.append([ddx, ddy, zs[i][1][zt] - zs[i][0][zt]])
                m = [U[3 + j, zt, X, r0 : r0 + 8, :] for j in range(3)]
                s, mag = strain_of(d, m)
                for p, (a, b) in enumerate(PAIRS):
                    T[p, zt, 8 * t : 8 * t + 8, :] = u[a][zt] * u[b][zt]
                    T[6 + p, zt, 8 * t : 8 * t + 8, :] = (0.5 if a == b else 0.25) * mag * s[p]
                MB[X, zt, 8 * t : 8 * t + 8, :] = mag
        for p in range(12):
            for zt in range(2):
                for t in range(2):
                    r = 8 * t
                    YF[p, zt, X, r : r + 8, :] = (
                        T[p, zt, r : r + 8, :] + 2.0 * T[p, zt, r + 1 : r + 9, :] + T[p, zt, r + 2 : r + 10, :])
        return 0


    def stage_y(X, _):
        for i in range(3):
            for zt in range(2):
                for t in range(3):
                    r = BASE - 1 + 8 * t
                    YV[i, zt, X, 8 * t : 8 * t + 8, :] = (
                        U[i, zt, X, r - 1 : r + 7, :] + 2.0 * U[i, zt, X, r : r + 8, :] + U[i, zt, X, r + 1 : r + 9, :])
        return 0


    def stage_v(X, _):
        turn = 127 - 6 * X
        x_in = jnp.logical_and(jnp.logical_or(X >= 2, gx > 0), jnp.logical_or(X < nx + 2, gx < ngx - 1))
        for t in range(3):
            rr_ = row + 8 * t
            y_in = jnp.logical_and(rr_ >= jnp.where(gy > 0, 0, 1), rr_ < jnp.where(gy < ngy - 1, ny + 2, ny + 1))
            inside = jnp.logical_and(y_in, x_in)
            for i in range(3):
                a = [YV[i, zt, X - 1, 8 * t : 8 * t + 8, :] + 2.0 * YV[i, zt, X, 8 * t : 8 * t + 8, :]
                     + YV[i, zt, X + 1, 8 * t : 8 * t + 8, :] for zt in range(2)]
                prev, nxt = zshift(a, pltpu.roll(VE[i, 8 * t : 8 * t + 8, :], turn, 1))
                for zt in range(2):
                    v = (1.0 / 64.0) * (prev[zt] + 2.0 * a[zt] + nxt[zt])
                    VH[i, zt, X, 8 * t : 8 * t + 8, :] = jnp.where(inside, v, 0.0)
        return 0


    def stage_c(X, _):
        turn = 127 - 6 * X
        for t in range(2):
            r = 8 * t
            v = [[VH[i, zt, X, r + 1 : r + 9, :] for zt in range(2)] for i in range(3)]
            zs = [zshift(v[i], pltpu.roll(VHE[i, r + 1 : r + 9, :], turn, 1)) for i in range(3)]
            fl = []
            for p in range(12):
                a = [YF[p, zt, X - 1, r : r + 8, :] + 2.0 * YF[p, zt, X, r : r + 8, :]
                     + YF[p, zt, X + 1, r : r + 8, :] for zt in range(2)]
                prev, nxt = zshift(a, pltpu.roll(ZE[p, r : r + 8, :], turn, 1))
                fl.append([(1.0 / 64.0) * (prev[zt] + 2.0 * a[zt] + nxt[zt]) for zt in range(2)])
            num = den = None
            for zt in range(2):
                d = []
                for i in range(3):
                    ddx = VH[i, zt, X + 1, r + 1 : r + 9, :] - VH[i, zt, X - 1, r + 1 : r + 9, :]
                    ddy = VH[i, zt, X, r + 2 : r + 10, :] - VH[i, zt, X, r : r + 8, :]
                    d.append([ddx, ddy, zs[i][1][zt] - zs[i][0][zt]])
                m = [U[3 + j, zt, X, BASE + r : BASE + r + 8, :] for j in range(3)]
                s, mag = strain_of(d, m)
                delta = jnp.exp2((-2.0 / 3.0) * jnp.log2(m[0] * m[1] * m[2]))
                nn = dd = None
                for p, (a, b) in enumerate(PAIRS):
                    w = 1.0 if a == b else 2.0
                    leo = fl[p][zt] - v[a][zt] * v[b][zt]
                    q = fl[6 + p][zt] - (2.0 if a == b else 1.0) * mag * s[p]
                    wq = q if a == b else w * q
                    n_, d_ = wq * leo, wq * q
                    nn = n_ if nn is None else nn + n_
                    dd = d_ if dd is None else dd + d_
                d2 = 2.0 * delta
                n_, d_ = d2 * nn, d2 * d2 * dd
                num = n_ if num is None else num + n_
                den = d_ if den is None else den + d_
                DM[X - 2, zt, r : r + 8, :] = delta * MB[X, zt, r + 1 : r + 9, :]
            at = X - 2 + nx * t
            ln = jnp.where(lane == at, jnp.sum(num, axis=1, keepdims=True), LN[gz])
            LN[gz] = jnp.where(lane == at + 2 * nx, jnp.sum(den, axis=1, keepdims=True), ln)
        return 0

    LN[gz] = z8
    got(2)
    got(3)
    for s in range(2):
        for f in range(6):
            for k in range(2):
                if f >= 3 and k == s:
                    continue
                y = (ny + k) if s else k - 2
                slab = 2 * f + k if f < 3 else 3 + f
                for zt in range(2):
                    U[f, zt, pl.ds(2, nx), BASE + y, :] = RY[s, slab, zt, :, :]
    lax.fori_loop(3, nx + 1, stage_a, 0)
    lax.fori_loop(2, nx + 2, stage_y, 0)
    lax.fori_loop(3, nx + 1, stage_v, 0)
    lax.fori_loop(4, nx, stage_c, 0)

    for n in range(4, 12):
        got(n)
    for sx in range(2):
        for sy in range(2):
            src = {}
            r = 0
            for f in range(6):
                for kx in range(2):
                    for ky in range(2):
                        if f >= 3 and (kx != 1 - sx or ky != 1 - sy):
                            continue
                        src[f, kx, ky] = r
                        r += 1
            for (f, kx, ky), r in src.items():
                X = (nx + 2 if sx else 0) + kx
                yr = (ny if sy else -2) + ky + BASE
                for zt in range(2):
                    U[f, zt, X, yr : yr + 1, :] = RC[2 * sx + sy, zt, r : r + 1, :]

    def ends(a, stage):
        lax.fori_loop(0, 4, lambda k, c: stage(jnp.where(k < 2, a + k, nx - a + k), c), 0)

    ends(1, stage_a)
    ends(0, stage_y)
    ends(1, stage_v)
    ends(2, stage_c)

    outs = []
    for zt in range(2):
        cp = pltpu.make_async_copy(DM.at[:, zt], dm_out.at[:, :, pl.ds(128 * zt, 128)], lsem.at[4 + zt])
        cp.start()
        outs.append(cp)

    cps = []
    for k in range(1, ngz):
        cp = pltpu.make_async_remote_copy(
            src_ref=LN.at[gz], dst_ref=LN.at[gz], send_sem=ssem.at[40 + k], recv_sem=rsem.at[40 + gz],
            device_id={"gz": lax.rem(gz + k, ngz)}, device_id_type=MESH)
        cp.start()
        cps.append(cp)
    for k in range(1, ngz):
        src = lax.rem(gz + k, ngz)
        pltpu.make_async_remote_copy(
            src_ref=LN.at[gz], dst_ref=LN.at[src], send_sem=ssem.at[40 + k], recv_sem=rsem.at[40 + src],
            device_id={"gz": src}, device_id_type=MESH).wait_recv()
    tot = LN[0]
    for k in range(1, ngz):
        tot = tot + LN[k]
    tot = tot * (1.0 / (nz * ngz))
    den = pltpu.roll(tot, 128 - 2 * nx, 1)
    line = tot / (den + 1e-06)
    valid = lane < 2 * nx
    peak = jnp.max(jnp.where(valid, line, -jnp.inf), axis=0, keepdims=True)
    peak = jnp.max(peak, axis=1, keepdims=True)

    RX[me_c] = jnp.broadcast_to(peak, (1, 128))
    for k in range(1, nxc):
        c, dev = xc_dev(k)
        cp = pltpu.make_async_remote_copy(
            src_ref=RX.at[me_c], dst_ref=RX.at[me_c], send_sem=ssem.at[44 + k], recv_sem=rsem.at[44 + me_c],
            device_id=dev, device_id_type=MESH)
        cp.start()
        cps.append(cp)
    for k in range(1, nxc):
        c, dev = xc_dev(k)
        pltpu.make_async_remote_copy(
            src_ref=RX.at[me_c], dst_ref=RX.at[c], send_sem=ssem.at[44 + k], recv_sem=rsem.at[44 + c],
            device_id=dev, device_id_type=MESH).wait_recv()
    peak = RX[0]
    for k in range(1, nxc):
        peak = jnp.maximum(peak, RX[k])
    RZ[xz] = peak
    for k in range(1, nzc):
        c, dev = z_dev(k)
        cp = pltpu.make_async_remote_copy(
            src_ref=RZ.at[xz], dst_ref=RZ.at[xz], send_sem=ssem.at[52 + k], recv_sem=rsem.at[52 + xz],
            device_id=dev, device_id_type=MESH)
        cp.start()
        cps.append(cp)
    for k in range(1, nzc):
        c, dev = z_dev(k)
        pltpu.make_async_remote_copy(
            src_ref=RZ.at[xz], dst_ref=RZ.at[c], send_sem=ssem.at[52 + k], recv_sem=rsem.at[52 + c],
            device_id=dev, device_id_type=MESH).wait_recv()
    peak = RZ[0]
    for k in range(1, nzc):
        peak = jnp.maximum(peak, RZ[k])

    half_out[...] = 0.5 * peak
    lt = line.T
    for t in range(2):
        line_out[:, 8 * t : 8 * t + 8] = lt[nx * t : nx * t + nx, :]
    for cp in outs:
        cp.wait()

    for cp in cps:
        cp.wait_send()
    for cp, cond in waits_send:
        if cond is None:
            cp.wait_send()
        else:
            pl.when(cond)(cp.wait_send)


def solution(mesh):
    sizes = tuple(mesh.shape[a] for a in ("gx", "gy", "gz"))
    ngx, ngy, ngz = sizes

    def per_device(velocity, metric):
        _, nx, ny, nz = velocity.shape
        vm = lambda *s: pltpu.VMEM(s, F32)
        dm, line, half = pl.pallas_call(
            functools.partial(kernel, sizes),
            out_shape=(jax.ShapeDtypeStruct((nx, ny, nz), F32), jax.ShapeDtypeStruct((nx, ny), F32),
                       jax.ShapeDtypeStruct((1, 128), F32)),
            in_specs=[pl.BlockSpec(memory_space=pl.ANY)] * 2,
            out_specs=(pl.BlockSpec(memory_space=pl.ANY),) + (pl.BlockSpec(memory_space=pltpu.VMEM),) * 2,
            scratch_shapes=[
                vm(6, 2, nx + 4, PITCH, 128),
                vm(6, 16, 128),
                vm(2, 9, 2, nx, 128),
                vm(2, 9, 2, nx, 128),
                vm(4, 2, 16, 128),
                vm(4, 2, 16, 128),
                vm(2, 6, 16, 128),
                vm(6, 32, 128),
                vm(2, 16, 128),
                vm(3, 2, 16, 128),
                vm(2, 16, 128),
                vm(3, 2, 16, 128),
                vm(3, 4, 8, 128),
                vm(2, 16, 128),
                vm(12, 24, 128),
                vm(3, 24, 128),
                vm(12, 16, 128),
                vm(3, 24, 128),
                vm(3, 24, 128),
                vm(12, 2, 24, 128),
                vm(12, 2, nx + 4, 16, 128),
                vm(3, 2, nx + 4, 24, 128),
                vm(3, 2, nx + 4, 24, 128),
                vm(nx + 4, 2, 24, 128),
                vm(nx, 2, 16, 128),
                vm(ngz, 8, 128),
                vm(2 * ngy, 1, 128),
                vm(ngx // 2, 1, 128),
                pltpu.SemaphoreType.DMA((6,)),
                pltpu.SemaphoreType.DMA((60,)),
                pltpu.SemaphoreType.DMA((60,)),
            ],
            compiler_params=pltpu.CompilerParams(collective_id=0, has_side_effects=True),
        )(velocity, metric)
        coefficient = jnp.minimum(line, half[0, 0])
        return coefficient[:, :, None] * dm, coefficient

    return jax.shard_map(
        per_device,
        mesh=mesh,
        in_specs=(P(None, "gx", "gy", "gz"), P(None, "gx", "gy", "gz")),
        out_specs=(P("gx", "gy", "gz"), P("gx", "gy")),
        check_vma=False,
    )
```

```python
import functools
import jax
import jax.numpy as jnp
from jax import lax
from jax.experimental import pallas as pl
from jax.experimental.pallas import tpu as pltpu
from jax.sharding import PartitionSpec as P

PAIRS = ((0, 0), (1, 1), (2, 2), (0, 1), (0, 2), (1, 2))
F32 = jnp.float32
MESH = pl.DeviceIdType.MESH
PITCH = 32
BASE = 8


def strain_of(diffs, m):
    g = [[m[j] * diffs[i][j] for j in range(3)] for i in range(3)]
    s = [g[a][a] if a == b else g[a][b] + g[b][a] for a, b in PAIRS]
    diag = s[0] * s[0] + s[1] * s[1] + s[2] * s[2]
    off = s[3] * s[3] + s[4] * s[4] + s[5] * s[5]
    return s, jnp.sqrt(0.5 * diag + 0.25 * off)


def kernel(sizes, vel, met, dm_out, line_out, half_out, U, O6, SY, RY, SC, RC, RO, ZG, SZX, RZX, SZY, RZY,
           RZC, SZG, TZ, UE, ZE, VE, VHE, T, YF, YV, VH, MB, DM, LN, RX, RZ, lsem, ssem, rsem):
    ngx, ngy, ngz = sizes
    nx = vel.shape[1]
    ny = vel.shape[2]
    nz = vel.shape[3]
    gx, gy, gz = lax.axis_index("gx"), lax.axis_index("gy"), lax.axis_index("gz")
    nzc = ngx // 2
    xlo, xz = lax.rem(gx, 2), lax.div(gx, 2)
    has = {("x", 0): gx > 0, ("x", 1): gx < ngx - 1, ("y", 0): gy > 0, ("y", 1): gy < ngy - 1}

    ins = []
    for zt in range(2):
        for k, ref in enumerate((vel, met)):
            cp = pltpu.make_async_copy(
                ref.at[:, :, :, pl.ds(128 * zt, 128)],
                U.at[pl.ds(3 * k, 3), zt, pl.ds(2, nx), pl.ds(BASE, ny), :],
                lsem.at[2 * zt + k],
            )
            cp.start()
            ins.append(cp)

    bar = pltpu.get_barrier_semaphore()

    def greet(dev):
        pl.semaphore_signal(bar, inc=1, device_id=dev, device_id_type=MESH)

    def dx(s):
        return gx + (1 if s else -1)

    def dy(s):
        return gy + (1 if s else -1)

    def gz_at(d):
        return lax.rem(gz + d + ngz, ngz)

    both = {(sx, sy): jnp.logical_and(has["x", sx], has["y", sy]) for sx in range(2) for sy in range(2)}
    for d in (-1, 1):
        greet({"gz": gz_at(d)})
    for s in range(2):
        @pl.when(has["y", s])
        def _():
            for d in (-1, 0, 1):
                greet({"gy": dy(s), "gz": gz_at(d)})

        @pl.when(has["x", s])
        def _():
            for d in (-1, 0, 1):
                greet({"gx": dx(s), "gz": gz_at(d)})

        for q in range(2):
            @pl.when(both[s, q])
            def _():
                for d in (-1, 0, 1):
                    greet({"gx": dx(s), "gy": dy(q), "gz": gz_at(d)})

    for k in range(2, ngz - 1):
        greet({"gz": gz_at(k)})

    nxc = 2 * ngy
    me_c = xlo * ngy + gy

    def xc_dev(k):
        c = lax.rem(me_c + k, nxc)
        return c, {"gx": xz * 2 + lax.div(c, ngy), "gy": lax.rem(c, ngy)}

    def z_dev(k):
        c = lax.rem(xz + k, nzc)
        return c, {"gx": c * 2 + xlo}

    for k in range(1, nxc):
        greet(xc_dev(k)[1])
    for k in range(1, nzc):
        greet(z_dev(k)[1])
    ex = has["x", 0].astype(jnp.int32) + has["x", 1].astype(jnp.int32)
    ey = has["y", 0].astype(jnp.int32) + has["y", 1].astype(jnp.int32)
    partners = 3 * (1 + ex) * (1 + ey) - 1 + max(ngz - 3, 0) + (nxc - 1) + (nzc - 1)

    z8 = jnp.zeros((8, 128), F32)
    for s in range(2):
        @pl.when(jnp.logical_not(has["x", s]))
        def _():
            for f in range(6):
                for zt in range(2):
                    for X in ((nx + 2, nx + 3) if s else (0, 1)):
                        for r in range(0, ny, 8):
                            U[f, zt, X, BASE + r : BASE + r + 8, :] = z8
            for d in range(3):
                RZX[d, s] = jnp.zeros(RZX.shape[2:], F32)

        @pl.when(jnp.logical_not(has["y", s]))
        def _():
            RY[s] = jnp.zeros(RY.shape[1:], F32)
            for d in range(3):
                RZY[d, s] = jnp.zeros(RZY.shape[2:], F32)

        for q in range(2):
            @pl.when(jnp.logical_not(both[s, q]))
            def _():
                RC[2 * s + q] = jnp.zeros(RC.shape[1:], F32)
                for d in range(3):
                    RZC[d, 2 * s + q] = z8

    for cp in ins:
        cp.wait()
    for s in range(2):
        for f in range(6):
            for k in range(2):
                if f >= 3 and k != s:
                    continue
                y = (ny - 2 + k) if s else k
                slab = 2 * f + k if f < 3 else 3 + f
                for zt in range(2):
                    SY[s, slab, zt, :, :] = U[f, zt, pl.ds(2, nx), BASE + y, :]

    pl.semaphore_wait(bar, partners)

    waits_send, waits_recv = [], {}

    def put(n, src, dst, dev, send_if=None, recv_if=None):
        cp = pltpu.make_async_remote_copy(
            src_ref=src, dst_ref=dst, send_sem=ssem.at[n], recv_sem=rsem.at[n],
            device_id=dev, device_id_type=MESH)
        if send_if is None:
            cp.start()
        else:
            pl.when(send_if)(cp.start)
        waits_send.append((cp, send_if))
        waits_recv[n] = (cp, recv_if)

    def got(n):
        cp, cond = waits_recv[n]
        if cond is None:
            cp.wait_recv()
        else:
            pl.when(cond)(cp.wait_recv)

    for s in range(2):
        put(2 + s, SY.at[s], RY.at[1 - s], {"gy": dy(s)}, has["y", s], has["y", 1 - s])

    lane = lax.broadcasted_iota(jnp.int32, (8, 128), 1)
    lx = lax.shift_right_logical(lane * 43, 8)
    lc = lane - 6 * lx
    row = lax.broadcasted_iota(jnp.int32, (8, 128), 0)
    half = lane < 64
    for f in range(6):
        for t in range(2):
            acc = z8
            rows = slice(BASE + 8 * t, BASE + 8 * t + 8)
            for X in range(2, nx + 2):
                a = jnp.where(half, U[f, 0, X, rows, :], U[f, 1, X, rows, :])
                acc = jnp.where(lx == X, pltpu.roll(a, (6 * X + 2) % 128, 1), acc)
            O6[f, 8 * t : 8 * t + 8, :] = acc

    for s in range(2):
        first = 6 * (nx if s else 2)
        for t in range(2):
            acc = z8
            for f in range(6):
                part = pltpu.roll(O6[f, 8 * t : 8 * t + 8, :], (12 * f - first) % 128, 1)
                acc = jnp.where(jnp.logical_and(lane >= 12 * f, lane < 12 * f + 12), part, acc)
            SZX[s, 8 * t : 8 * t + 8, :] = acc
        y = ny - 2 if s else 0
        for f in range(6):
            SZY[s, 2 * f : 2 * f + 2, :] = O6[f, y : y + 2, :]
        SZY[s, 12:16, :] = z8[0:4]

    def corner_rows(out, sx, sy):
        r = 0
        for f in range(6):
            for kx in range(2):
                for ky in range(2):
                    if f >= 3 and (kx != sx or ky != sy):
                        continue
                    if out:
                        X = (nx if sx else 2) + kx
                        y = (ny - 2 if sy else 0) + ky
                    else:
                        X = (nx + 2 if sx else 0) + kx
                        y = (ny if sy else -2) + ky
                    yield r, f, X, y + BASE
                    r += 1

    for sx in range(2):
        for sy in range(2):
            for r, f, X, yr in corner_rows(True, sx, sy):
                for zt in range(2):
                    SC[2 * sx + sy, zt, r : r + 1, :] = U[f, zt, X, yr : yr + 1, :]


    for s in range(2):
        put(s, O6, RO.at[1 - s], {"gz": gz_at(1 if s else -1)})
    for i, d in enumerate((-1, 0, 1)):
        o = 2 - i
        for s in range(2):
            put(12 + 2 * i + s, SZY.at[s], RZY.at[o, 1 - s], {"gy": dy(s), "gz": gz_at(d)},
                has["y", s], has["y", 1 - s])
            put(18 + 2 * i + s, SZX.at[s], RZX.at[o, 1 - s], {"gx": dx(s), "gz": gz_at(d)},
                has["x", s], has["x", 1 - s])
        for sx in range(2):
            for sy in range(2):
                put(24 + 4 * i + 2 * sx + sy, SZX.at[sx, pl.ds(ny - 8 if sy else 0, 8), :],
                    RZC.at[o, 2 * (1 - sx) + 1 - sy],
                    {"gx": dx(sx), "gy": dy(sy), "gz": gz_at(d)},
                    both[sx, sy], both[1 - sx, 1 - sy])
    def comb(left, own, right):
        return jnp.where(lc < 2, left, jnp.where(lc == 2, own, pltpu.roll(jnp.where(lc == 1, own, right), 2, 1)))

    for n in (0, 1, *range(12, 36)):
        got(n)
    zx, zc = {}, {}
    for s in range(2):
        for t in range(2):
            rows = slice(8 * t, 8 * t + 8)
            zx[s, t] = comb(RZX[0, s, rows, :], RZX[1, s, rows, :], RZX[2, s, rows, :])
            SZG[s, rows, :] = comb(RZY[0, s, rows, :], RZY[1, s, rows, :], RZY[2, s, rows, :])
    for c in range(4):
        zc[c] = comb(RZC[0, c], RZC[1, c], RZC[2, c])
    for f in range(6):
        ZG[f, 0:8, :] = z8
        ZG[f, 24:32, :] = z8
        for t in range(2):
            rows = slice(8 * t, 8 * t + 8)
            z = comb(RO[0, f, rows, :], O6[f, rows, :], RO[1, f, rows, :])
            for s in range(2):
                at = 6 * (nx + 2) if s else 0
                part = pltpu.roll(zx[s, t], (at - 12 * f) % 128, 1)
                z = jnp.where(jnp.logical_and(lane >= at, lane < at + 12), part, z)
            ZG[f, BASE + 8 * t : BASE + 8 * t + 8, :] = z
        for sy in range(2):
            yr = BASE + (ny if sy else -2)
            z = SZG[sy, 2 * f : 2 * f + 2, :]
            for sx in range(2):
                at = 6 * (nx + 2) if sx else 0
                part = pltpu.roll(zc[2 * sx + sy], (at - 12 * f) % 128, 1)
                part = part[0:2] if sy else part[6:8]
                lane2 = lane[0:2]
                z = jnp.where(jnp.logical_and(lane2 >= at, lane2 < at + 12), part, z)
            ZG[f, yr : yr + 2, :] = z

    def edge(a):
        return jnp.where(lc == 0, pltpu.roll(a, 124, 1), a)

    def xsum(a):
        return pltpu.roll(a, 6, 1) + 2.0 * a + pltpu.roll(a, 122, 1)

    xd = lambda a: pltpu.roll(a, 122, 1) - pltpu.roll(a, 6, 1)
    zd = lambda a: pltpu.roll(a, 127, 1) - pltpu.roll(a, 1, 1)
    for t in range(3):
        r0 = BASE - 1 + 8 * t
        at = lambda f, d: ZG[f, r0 + d : r0 + d + 8, :]
        u = [at(i, 0) for i in range(3)]
        up = [at(i, 1) for i in range(3)]
        dn = [at(i, -1) for i in range(3)]
        m = [at(3 + j, 0) for j in range(3)]
        d = [[xd(u[i]), up[i] - dn[i], zd(u[i])] for i in range(3)]
        s, mag = strain_of(d, m)
        for p, (a, b) in enumerate(PAIRS):
            TZ[p, 8 * t : 8 * t + 8, :] = u[a] * u[b]
            TZ[6 + p, 8 * t : 8 * t + 8, :] = (0.5 if a == b else 0.25) * mag * s[p]
        for i in range(3):
            UE[i, 8 * t : 8 * t + 8, :] = edge(u[i])
            v = xsum(up[i] + dn[i] + 2.0 * u[i])
            VE[i, 8 * t : 8 * t + 8, :] = edge(v)
            vz = (1.0 / 64.0) * (pltpu.roll(v, 1, 1) + 2.0 * v + pltpu.roll(v, 127, 1))
            VHE[i, 8 * t : 8 * t + 8, :] = edge(vz)
    for p in range(12):
        for t in range(2):
            a = TZ[p, 8 * t : 8 * t + 8, :] + 2.0 * TZ[p, 8 * t + 1 : 8 * t + 9, :] + TZ[p, 8 * t + 2 : 8 * t + 10, :]
            ZE[p, 8 * t : 8 * t + 8, :] = edge(xsum(a))

    first_lane, last_lane = lane == 0, lane == 127

    def zshift(a, e):
        p0, p1 = pltpu.roll(a[0], 1, 1), pltpu.roll(a[1], 1, 1)
        n0, n1 = pltpu.roll(a[0], 127, 1), pltpu.roll(a[1], 127, 1)
        prev = (jnp.where(first_lane, e, p0), jnp.where(first_lane, p0, p1))
        nxt = (jnp.where(last_lane, n1, n0), jnp.where(last_lane, e, n1))
        return prev, nxt

    def stage_a(X, _):
        turn = 127 - 6 * X
        for t in range(3):
            r0 = BASE - 1 + 8 * t
            u = [[U[i, zt, X, r0 : r0 + 8, :] for zt in range(2)] for i in range(3)]
            zs = [zshift(u[i], pltpu.roll(UE[i, 8 * t : 8 * t + 8, :], turn, 1)) for i in range(3)]
            for zt in range(2):
                d = []
                for i in range(3):
                    ddx = U[i, zt, X + 1, r0 : r0 + 8, :] - U[i, zt, X - 1, r0 : r0 + 8, :]
                    ddy = U[i, zt, X, r0 + 1 : r0 + 9, :] - U[i, zt, X, r0 - 1 : r0 + 7, :]
                    d.append([ddx, ddy, zs[i][1][zt] - zs[i][0][zt]])
                m = [U[3 + j, zt, X, r0 : r0 + 8, :] for j in range(3)]
                s, mag = strain_of(d, m)
                for p, (a, b) in enumerate(PAIRS):
                    T[p, zt, 8 * t : 8 * t + 8, :] = u[a][zt] * u[b][zt]
                    T[6 + p, zt, 8 * t : 8 * t + 8, :] = (0.5 if a == b else 0.25) * mag * s[p]
                MB[X, zt, 8 * t : 8 * t + 8, :] = mag
        for p in range(12):
            for zt in range(2):
                for t in range(2):
                    r = 8 * t
                    YF[p, zt, X, r : r + 8, :] = (
                        T[p, zt, r : r + 8, :] + 2.0 * T[p, zt, r + 1 : r + 9, :] + T[p, zt, r + 2 : r + 10, :])
        return 0


    def stage_y(X, _):
        for i in range(3):
            for zt in range(2):
                for t in range(3):
                    r = BASE - 1 + 8 * t
                    YV[i, zt, X, 8 * t : 8 * t + 8, :] = (
                        U[i, zt, X, r - 1 : r + 7, :] + 2.0 * U[i, zt, X, r : r + 8, :] + U[i, zt, X, r + 1 : r + 9, :])
        return 0


    def stage_v(X, _):
        turn = 127 - 6 * X
        x_in = jnp.logical_and(jnp.logical_or(X >= 2, gx > 0), jnp.logical_or(X < nx + 2, gx < ngx - 1))
        for t in range(3):
            rr_ = row + 8 * t
            y_in = jnp.logical_and(rr_ >= jnp.where(gy > 0, 0, 1), rr_ < jnp.where(gy < ngy - 1, ny + 2, ny + 1))
            inside = jnp.logical_and(y_in, x_in)
            for i in range(3):
                a = [YV[i, zt, X - 1, 8 * t : 8 * t + 8, :] + 2.0 * YV[i, zt, X, 8 * t : 8 * t + 8, :]
                     + YV[i, zt, X + 1, 8 * t : 8 * t + 8, :] for zt in range(2)]
                prev, nxt = zshift(a, pltpu.roll(VE[i, 8 * t : 8 * t + 8, :], turn, 1))
                for zt in range(2):
                    v = (1.0 / 64.0) * (prev[zt] + 2.0 * a[zt] + nxt[zt])
                    VH[i, zt, X, 8 * t : 8 * t + 8, :] = jnp.where(inside, v, 0.0)
        return 0


    def stage_c(X, _):
        turn = 127 - 6 * X
        for t in range(2):
            r = 8 * t
            v = [[VH[i, zt, X, r + 1 : r + 9, :] for zt in range(2)] for i in range(3)]
            zs = [zshift(v[i], pltpu.roll(VHE[i, r + 1 : r + 9, :], turn, 1)) for i in range(3)]
            fl = []
            for p in range(12):
                a = [YF[p, zt, X - 1, r : r + 8, :] + 2.0 * YF[p, zt, X, r : r + 8, :]
                     + YF[p, zt, X + 1, r : r + 8, :] for zt in range(2)]
                prev, nxt = zshift(a, pltpu.roll(ZE[p, r : r + 8, :], turn, 1))
                fl.append([(1.0 / 64.0) * (prev[zt] + 2.0 * a[zt] + nxt[zt]) for zt in range(2)])
            num = den = None
            for zt in range(2):
                d = []
                for i in range(3):
                    ddx = VH[i, zt, X + 1, r + 1 : r + 9, :] - VH[i, zt, X - 1, r + 1 : r + 9, :]
                    ddy = VH[i, zt, X, r + 2 : r + 10, :] - VH[i, zt, X, r : r + 8, :]
                    d.append([ddx, ddy, zs[i][1][zt] - zs[i][0][zt]])
                m = [U[3 + j, zt, X, BASE + r : BASE + r + 8, :] for j in range(3)]
                s, mag = strain_of(d, m)
                delta = jnp.exp2((-2.0 / 3.0) * jnp.log2(m[0] * m[1] * m[2]))
                nn = dd = None
                for p, (a, b) in enumerate(PAIRS):
                    w = 1.0 if a == b else 2.0
                    leo = fl[p][zt] - v[a][zt] * v[b][zt]
                    q = fl[6 + p][zt] - (2.0 if a == b else 1.0) * mag * s[p]
                    wq = q if a == b else w * q
                    n_, d_ = wq * leo, wq * q
                    nn = n_ if nn is None else nn + n_
                    dd = d_ if dd is None else dd + d_
                d2 = 2.0 * delta
                n_, d_ = d2 * nn, d2 * d2 * dd
                num = n_ if num is None else num + n_
                den = d_ if den is None else den + d_
                DM[X - 2, zt, r : r + 8, :] = delta * MB[X, zt, r + 1 : r + 9, :]
            at = X - 2 + nx * t
            ln = jnp.where(lane == at, jnp.sum(num, axis=1, keepdims=True), LN[gz])
            LN[gz] = jnp.where(lane == at + 2 * nx, jnp.sum(den, axis=1, keepdims=True), ln)
        return 0

    LN[gz] = z8
    got(2)
    got(3)
    rr = pl.ds(BASE, ny)
    for s in range(2):
        far, near = (nx, nx + 1) if s else (3, 2)
        gfar, gnear = (0, 1) if s else (nx + 3, nx + 2)
        put(4 + s, U.at[:, :, near, rr, :], U.at[:, :, gnear, rr, :], {"gx": dx(s)},
            has["x", s], has["x", 1 - s])
        put(6 + s, U.at[pl.ds(0, 3), :, far, rr, :], U.at[pl.ds(0, 3), :, gfar, rr, :],
            {"gx": dx(s)}, has["x", s], has["x", 1 - s])
    for sx in range(2):
        for sy in range(2):
            put(8 + 2 * sx + sy, SC.at[2 * sx + sy], RC.at[2 * (1 - sx) + 1 - sy],
                {"gx": dx(sx), "gy": dy(sy)}, both[sx, sy], both[1 - sx, 1 - sy])

    for s in range(2):
        for f in range(6):
            for k in range(2):
                if f >= 3 and k == s:
                    continue
                y = (ny + k) if s else k - 2
                slab = 2 * f + k if f < 3 else 3 + f
                for zt in range(2):
                    U[f, zt, pl.ds(2, nx), BASE + y, :] = RY[s, slab, zt, :, :]
    lax.fori_loop(3, nx + 1, stage_a, 0)
    lax.fori_loop(2, nx + 2, stage_y, 0)
    lax.fori_loop(3, nx + 1, stage_v, 0)
    lax.fori_loop(4, nx, stage_c, 0)

    for n in range(4, 12):
        got(n)
    for sx in range(2):
        for sy in range(2):
            src = {}
            r = 0
            for f in range(6):
                for kx in range(2):
                    for ky in range(2):
                        if f >= 3 and (kx != 1 - sx or ky != 1 - sy):
                            continue
                        src[f, kx, ky] = r
                        r += 1
            for (f, kx, ky), r in src.items():
                X = (nx + 2 if sx else 0) + kx
                yr = (ny if sy else -2) + ky + BASE
                for zt in range(2):
                    U[f, zt, X, yr : yr + 1, :] = RC[2 * sx + sy, zt, r : r + 1, :]

    def ends(a, stage):
        lax.fori_loop(0, 4, lambda k, c: stage(jnp.where(k < 2, a + k, nx - a + k), c), 0)

    ends(1, stage_a)
    ends(0, stage_y)
    ends(1, stage_v)
    ends(2, stage_c)

    outs = []
    for zt in range(2):
        cp = pltpu.make_async_copy(DM.at[:, zt], dm_out.at[:, :, pl.ds(128 * zt, 128)], lsem.at[4 + zt])
        cp.start()
        outs.append(cp)

    cps = []
    for k in range(1, ngz):
        cp = pltpu.make_async_remote_copy(
            src_ref=LN.at[gz], dst_ref=LN.at[gz], send_sem=ssem.at[40 + k], recv_sem=rsem.at[40 + gz],
            device_id={"gz": lax.rem(gz + k, ngz)}, device_id_type=MESH)
        cp.start()
        cps.append(cp)
    for k in range(1, ngz):
        src = lax.rem(gz + k, ngz)
        pltpu.make_async_remote_copy(
            src_ref=LN.at[gz], dst_ref=LN.at[src], send_sem=ssem.at[40 + k], recv_sem=rsem.at[40 + src],
            device_id={"gz": src}, device_id_type=MESH).wait_recv()
    tot = LN[0]
    for k in range(1, ngz):
        tot = tot + LN[k]
    tot = tot * (1.0 / (nz * ngz))
    den = pltpu.roll(tot, 128 - 2 * nx, 1)
    line = tot / (den + 1e-06)
    valid = lane < 2 * nx
    peak = jnp.max(jnp.where(valid, line, -jnp.inf), axis=0, keepdims=True)
    peak = jnp.max(peak, axis=1, keepdims=True)

    RX[me_c] = jnp.broadcast_to(peak, (1, 128))
    for k in range(1, nxc):
        c, dev = xc_dev(k)
        cp = pltpu.make_async_remote_copy(
            src_ref=RX.at[me_c], dst_ref=RX.at[me_c], send_sem=ssem.at[44 + k], recv_sem=rsem.at[44 + me_c],
            device_id=dev, device_id_type=MESH)
        cp.start()
        cps.append(cp)
    for k in range(1, nxc):
        c, dev = xc_dev(k)
        pltpu.make_async_remote_copy(
            src_ref=RX.at[me_c], dst_ref=RX.at[c], send_sem=ssem.at[44 + k], recv_sem=rsem.at[44 + c],
            device_id=dev, device_id_type=MESH).wait_recv()
    peak = RX[0]
    for k in range(1, nxc):
        peak = jnp.maximum(peak, RX[k])
    RZ[xz] = peak
    for k in range(1, nzc):
        c, dev = z_dev(k)
        cp = pltpu.make_async_remote_copy(
            src_ref=RZ.at[xz], dst_ref=RZ.at[xz], send_sem=ssem.at[52 + k], recv_sem=rsem.at[52 + xz],
            device_id=dev, device_id_type=MESH)
        cp.start()
        cps.append(cp)
    for k in range(1, nzc):
        c, dev = z_dev(k)
        pltpu.make_async_remote_copy(
            src_ref=RZ.at[xz], dst_ref=RZ.at[c], send_sem=ssem.at[52 + k], recv_sem=rsem.at[52 + c],
            device_id=dev, device_id_type=MESH).wait_recv()
    peak = RZ[0]
    for k in range(1, nzc):
        peak = jnp.maximum(peak, RZ[k])

    half_out[...] = 0.5 * peak
    lt = line.T
    for t in range(2):
        line_out[:, 8 * t : 8 * t + 8] = lt[nx * t : nx * t + nx, :]
    for cp in outs:
        cp.wait()

    for cp in cps:
        cp.wait_send()
    for cp, cond in waits_send:
        if cond is None:
            cp.wait_send()
        else:
            pl.when(cond)(cp.wait_send)


def solution(mesh):
    sizes = tuple(mesh.shape[a] for a in ("gx", "gy", "gz"))
    ngx, ngy, ngz = sizes

    def per_device(velocity, metric):
        _, nx, ny, nz = velocity.shape
        vm = lambda *s: pltpu.VMEM(s, F32)
        dm, line, half = pl.pallas_call(
            functools.partial(kernel, sizes),
            out_shape=(vm(nx, ny, nz), vm(nx, ny), vm(1, 128)),
            in_specs=[pl.BlockSpec(memory_space=pl.ANY)] * 2,
            out_specs=(pl.BlockSpec(memory_space=pl.ANY),) + (pl.BlockSpec(memory_space=pltpu.VMEM),) * 2,
            scratch_shapes=[
                vm(6, 2, nx + 4, PITCH, 128),
                vm(6, 16, 128),
                vm(2, 9, 2, nx, 128),
                vm(2, 9, 2, nx, 128),
                vm(4, 2, 16, 128),
                vm(4, 2, 16, 128),
                vm(2, 6, 16, 128),
                vm(6, 32, 128),
                vm(2, 16, 128),
                vm(3, 2, 16, 128),
                vm(2, 16, 128),
                vm(3, 2, 16, 128),
                vm(3, 4, 8, 128),
                vm(2, 16, 128),
                vm(12, 24, 128),
                vm(3, 24, 128),
                vm(12, 16, 128),
                vm(3, 24, 128),
                vm(3, 24, 128),
                vm(12, 2, 24, 128),
                vm(12, 2, nx + 4, 16, 128),
                vm(3, 2, nx + 4, 24, 128),
                vm(3, 2, nx + 4, 24, 128),
                vm(nx + 4, 2, 24, 128),
                vm(nx, 2, 16, 128),
                vm(ngz, 8, 128),
                vm(2 * ngy, 1, 128),
                vm(ngx // 2, 1, 128),
                pltpu.SemaphoreType.DMA((6,)),
                pltpu.SemaphoreType.DMA((60,)),
                pltpu.SemaphoreType.DMA((60,)),
            ],
            compiler_params=pltpu.CompilerParams(collective_id=0, has_side_effects=True),
        )(velocity, metric)
        coefficient = jnp.minimum(line, half[0, 0])
        return coefficient[:, :, None] * dm, coefficient

    return jax.shard_map(
        per_device,
        mesh=mesh,
        in_specs=(P(None, "gx", "gy", "gz"), P(None, "gx", "gy", "gz")),
        out_specs=(P("gx", "gy", "gz"), P("gx", "gy")),
        check_vma=False,
    )
```

```python
import functools
import jax
import jax.numpy as jnp
from jax import lax
from jax.experimental import pallas as pl
from jax.experimental.pallas import tpu as pltpu
from jax.sharding import PartitionSpec as P

PAIRS = ((0, 0), (1, 1), (2, 2), (0, 1), (0, 2), (1, 2))
F32 = jnp.float32
MESH = pl.DeviceIdType.MESH
PITCH = 32
BASE = 8
UA, UY, UV, UC, UE4 = 2, 4, 7, 4, 4


def strain_of(diffs, m):
    g = [[m[j] * diffs[i][j] for j in range(3)] for i in range(3)]
    s = [g[a][a] if a == b else g[a][b] + g[b][a] for a, b in PAIRS]
    diag = s[0] * s[0] + s[1] * s[1] + s[2] * s[2]
    off = s[3] * s[3] + s[4] * s[4] + s[5] * s[5]
    return s, jnp.sqrt(0.5 * diag + 0.25 * off)


def kernel(sizes, vel, met, dm_out, line_out, half_out, U, O6, SY, RY, SC, RC, RO, ZG, SZX, RZX, SZY, RZY,
           SZC, RZC, ZC, SZG, TZ, UE, ZE, VE, VHE, T, YF, YV, VH, MB, DM, NP, LN, RX, RZ, lsem, ssem, rsem):
    ngx, ngy, ngz = sizes
    nx = vel.shape[1]
    ny = vel.shape[2]
    nz = vel.shape[3]
    gx, gy, gz = lax.axis_index("gx"), lax.axis_index("gy"), lax.axis_index("gz")
    nzc = ngx // 2
    xlo, xz = lax.rem(gx, 2), lax.div(gx, 2)
    has = {("x", 0): gx > 0, ("x", 1): gx < ngx - 1, ("y", 0): gy > 0, ("y", 1): gy < ngy - 1}

    ins = []
    for zt in range(2):
        for k, ref in enumerate((vel, met)):
            cp = pltpu.make_async_copy(
                ref.at[:, :, :, pl.ds(128 * zt, 128)],
                U.at[pl.ds(3 * k, 3), zt, pl.ds(2, nx), pl.ds(BASE, ny), :],
                lsem.at[2 * zt + k],
            )
            cp.start()
            ins.append(cp)

    bar = pltpu.get_barrier_semaphore()

    def greet(dev):
        pl.semaphore_signal(bar, inc=1, device_id=dev, device_id_type=MESH)

    def dx(s):
        return gx + (1 if s else -1)

    def dy(s):
        return gy + (1 if s else -1)

    def gz_at(d):
        return lax.rem(gz + d + ngz, ngz)

    both = {(sx, sy): jnp.logical_and(has["x", sx], has["y", sy]) for sx in range(2) for sy in range(2)}
    for d in (-1, 1):
        greet({"gz": gz_at(d)})
    for s in range(2):
        @pl.when(has["y", s])
        def _():
            for d in (-1, 0, 1):
                greet({"gy": dy(s), "gz": gz_at(d)})

        @pl.when(has["x", s])
        def _():
            for d in (-1, 0, 1):
                greet({"gx": dx(s), "gz": gz_at(d)})

        for q in range(2):
            @pl.when(both[s, q])
            def _():
                for d in (-1, 0, 1):
                    greet({"gx": dx(s), "gy": dy(q), "gz": gz_at(d)})

    for k in range(2, ngz - 1):
        greet({"gz": gz_at(k)})

    nxc = 2 * ngy
    me_c = xlo * ngy + gy

    def xc_dev(k):
        c = lax.rem(me_c + k, nxc)
        return c, {"gx": xz * 2 + lax.div(c, ngy), "gy": lax.rem(c, ngy)}

    def z_dev(k):
        c = lax.rem(xz + k, nzc)
        return c, {"gx": c * 2 + xlo}

    for k in range(1, nxc):
        greet(xc_dev(k)[1])
    for k in range(1, nzc):
        greet(z_dev(k)[1])
    ex = has["x", 0].astype(jnp.int32) + has["x", 1].astype(jnp.int32)
    ey = has["y", 0].astype(jnp.int32) + has["y", 1].astype(jnp.int32)
    partners = 3 * (1 + ex) * (1 + ey) - 1 + max(ngz - 3, 0) + (nxc - 1) + (nzc - 1)

    z8 = jnp.zeros((8, 128), F32)
    for s in range(2):
        @pl.when(jnp.logical_not(has["x", s]))
        def _():
            for f in range(6):
                for zt in range(2):
                    for X in ((nx + 2, nx + 3) if s else (0, 1)):
                        for r in range(0, ny, 8):
                            U[f, zt, X, BASE + r : BASE + r + 8, :] = z8
            for d in range(3):
                RZX[d, s] = jnp.zeros(RZX.shape[2:], F32)

        @pl.when(jnp.logical_not(has["y", s]))
        def _():
            RY[s] = jnp.zeros(RY.shape[1:], F32)
            for d in range(3):
                RZY[d, s] = jnp.zeros(RZY.shape[2:], F32)

        for q in range(2):
            @pl.when(jnp.logical_not(both[s, q]))
            def _():
                RC[2 * s + q] = jnp.zeros(RC.shape[1:], F32)
                for d in range(3):
                    RZC[d, 2 * s + q] = jnp.zeros(RZC.shape[2:], F32)

    for cp in ins:
        cp.wait()
    for s in range(2):
        for f in range(6):
            for k in range(2):
                if f >= 3 and k != s:
                    continue
                y = (ny - 2 + k) if s else k
                slab = 2 * f + k if f < 3 else 3 + f
                for zt in range(2):
                    SY[s, slab, zt, :, :] = U[f, zt, pl.ds(2, nx), BASE + y, :]

    pl.semaphore_wait(bar, partners)

    waits_send, waits_recv = [], {}

    def put(n, src, dst, dev, send_if=None, recv_if=None):
        cp = pltpu.make_async_remote_copy(
            src_ref=src, dst_ref=dst, send_sem=ssem.at[n], recv_sem=rsem.at[n],
            device_id=dev, device_id_type=MESH)
        if send_if is None:
            cp.start()
        else:
            pl.when(send_if)(cp.start)
        waits_send.append((cp, send_if))
        waits_recv[n] = (cp, recv_if)

    def got(n):
        cp, cond = waits_recv[n]
        if cond is None:
            cp.wait_recv()
        else:
            pl.when(cond)(cp.wait_recv)

    for s in range(2):
        put(2 + s, SY.at[s], RY.at[1 - s], {"gy": dy(s)}, has["y", s], has["y", 1 - s])

    lane = lax.broadcasted_iota(jnp.int32, (8, 128), 1)
    lx = lax.shift_right_logical(lane * 43, 8)
    lc = lane - 6 * lx
    row = lax.broadcasted_iota(jnp.int32, (8, 128), 0)
    half = lane < 64
    for f in range(6):
        for t in range(2):
            acc = z8
            rows = slice(BASE + 8 * t, BASE + 8 * t + 8)
            for X in range(2, nx + 2):
                a = jnp.where(half, U[f, 0, X, rows, :], U[f, 1, X, rows, :])
                acc = jnp.where(lx == X, pltpu.roll(a, (6 * X + 2) % 128, 1), acc)
            O6[f, 8 * t : 8 * t + 8, :] = acc

    def x_at(f, t):
        return 54 * t + (12 * f if f < 3 else 18 + 6 * f)

    def x_lanes(lanes, at, f):
        return jnp.logical_and(lanes >= at, lanes < at + (12 if f < 3 else 6))

    for s in range(2):
        acc = z8
        for t in range(2):
            for f in range(6):
                first = 6 * ((nx + (f >= 3)) if s else 2)
                part = pltpu.roll(O6[f, 8 * t : 8 * t + 8, :], (x_at(f, t) - first) % 128, 1)
                acc = jnp.where(x_lanes(lane, x_at(f, t), f), part, acc)
        SZX[s] = acc
        for sy in range(2):
            for k in range(2):
                SZC[2 * s + sy, k] = acc[6 + k : 7 + k] if sy else acc[k : k + 1]
        y = ny - 2 if s else 0
        for f in range(6):
            SZY[s, 2 * f : 2 * f + 2, :] = O6[f, y : y + 2, :]
        SZY[s, 12:16, :] = z8[0:4]

    def corner_rows(sx, sy):
        rows = [(f, kx, ky) for f in range(6) for kx in range(2) for ky in range(2)
                if (kx == sx and ky == sy) or (f < 3 and (kx == sx or ky == sy))]
        return [(12 * zt + r, zt, *q) for zt in range(2) for r, q in enumerate(rows)]

    for sx in range(2):
        for sy in range(2):
            for r, zt, f, kx, ky in corner_rows(sx, sy):
                X, yr = (nx if sx else 2) + kx, (ny - 2 if sy else 0) + ky + BASE
                SC[2 * sx + sy, r : r + 1, :] = U[f, zt, X, yr : yr + 1, :]

    for s in range(2):
        put(s, O6, RO.at[1 - s], {"gz": gz_at(1 if s else -1)})
    for i, d in enumerate((-1, 0, 1)):
        o = 2 - i
        for s in range(2):
            put(12 + 2 * i + s, SZY.at[s], RZY.at[o, 1 - s], {"gy": dy(s), "gz": gz_at(d)},
                has["y", s], has["y", 1 - s])
            put(18 + 2 * i + s, SZX.at[s], RZX.at[o, 1 - s], {"gx": dx(s), "gz": gz_at(d)},
                has["x", s], has["x", 1 - s])
        for sx in range(2):
            for sy in range(2):
                put(24 + 4 * i + 2 * sx + sy, SZC.at[2 * sx + sy],
                    RZC.at[o, 2 * (1 - sx) + 1 - sy],
                    {"gx": dx(sx), "gy": dy(sy), "gz": gz_at(d)},
                    both[sx, sy], both[1 - sx, 1 - sy])
    def comb(left, own, right):
        return jnp.where(lc < 2, left, jnp.where(lc == 2, own, pltpu.roll(jnp.where(lc == 1, own, right), 2, 1)))

    got(0)
    got(1)
    for n in (12,13,14,15,16,17):
        got(n)
    rr = pl.ds(BASE, ny)
    for s in range(2):
        far, near = (nx, nx + 1) if s else (3, 2)
        gfar, gnear = (0, 1) if s else (nx + 3, nx + 2)
        put(4 + s, U.at[:, :, near, rr, :], U.at[:, :, gnear, rr, :], {"gx": dx(s)},
            has["x", s], has["x", 1 - s])
        put(6 + s, U.at[pl.ds(0, 3), :, far, rr, :], U.at[pl.ds(0, 3), :, gfar, rr, :],
            {"gx": dx(s)}, has["x", s], has["x", 1 - s])
    for sx in range(2):
        for sy in range(2):
            put(8 + 2 * sx + sy, SC.at[2 * sx + sy], RC.at[2 * (1 - sx) + 1 - sy],
                {"gx": dx(sx), "gy": dy(sy)}, both[sx, sy], both[1 - sx, 1 - sy])
    for n in range(18, 36):
        got(n)
    zx = [comb(RZX[0, s], RZX[1, s], RZX[2, s]) for s in range(2)]
    for s in range(2):
        for t in range(2):
            rows = slice(8 * t, 8 * t + 8)
            SZG[s, rows, :] = comb(RZY[0, s, rows, :], RZY[1, s, rows, :], RZY[2, s, rows, :])
    lane1 = lc[0:1]
    for c in range(4):
        ZC[c] = z8
        for k in range(2):
            left, own, right = (RZC[d, c, k] for d in range(3))
            ZC[c, k : k + 1, :] = jnp.where(lane1 < 2, left, jnp.where(
                lane1 == 2, own, pltpu.roll(jnp.where(lane1 == 1, own, right), 2, 1)))

    def x_place(sx, f):
        return 6 * (nx + 2) if sx else (0 if f < 3 else 6)

    for f in range(6):
        ZG[f, 0:8, :] = z8
        ZG[f, 24:32, :] = z8
        for t in range(2):
            rows = slice(8 * t, 8 * t + 8)
            z = comb(RO[0, f, rows, :], O6[f, rows, :], RO[1, f, rows, :])
            for sx in range(2):
                at = x_place(sx, f)
                part = pltpu.roll(zx[sx], (at - x_at(f, t)) % 128, 1)
                z = jnp.where(x_lanes(lane, at, f), part, z)
            ZG[f, BASE + 8 * t : BASE + 8 * t + 8, :] = z
        for sy in range(2):
            yr = BASE + (ny if sy else -2)
            z = SZG[sy, 2 * f : 2 * f + 2, :]
            for sx in range(2):
                at = x_place(sx, f)
                part = pltpu.roll(ZC[2 * sx + sy], (at - x_at(f, 1 - sy)) % 128, 1)[0:2]
                z = jnp.where(x_lanes(lane[0:2], at, f), part, z)
            ZG[f, yr : yr + 2, :] = z

    def edge(a):
        return jnp.where(lc == 0, pltpu.roll(a, 124, 1), a)

    def xsum(a):
        return pltpu.roll(a, 6, 1) + 2.0 * a + pltpu.roll(a, 122, 1)

    xd = lambda a: pltpu.roll(a, 122, 1) - pltpu.roll(a, 6, 1)
    zd = lambda a: pltpu.roll(a, 127, 1) - pltpu.roll(a, 1, 1)
    for t in range(3):
        r0 = BASE - 1 + 8 * t
        at = lambda f, d: ZG[f, r0 + d : r0 + d + 8, :]
        u = [at(i, 0) for i in range(3)]
        up = [at(i, 1) for i in range(3)]
        dn = [at(i, -1) for i in range(3)]
        m = [at(3 + j, 0) for j in range(3)]
        d = [[xd(u[i]), up[i] - dn[i], zd(u[i])] for i in range(3)]
        s, mag = strain_of(d, m)
        for p, (a, b) in enumerate(PAIRS):
            TZ[p, 8 * t : 8 * t + 8, :] = u[a] * u[b]
            TZ[6 + p, 8 * t : 8 * t + 8, :] = (0.5 if a == b else 0.25) * mag * s[p]
        for i in range(3):
            UE[i, 8 * t : 8 * t + 8, :] = edge(u[i])
            v = xsum(up[i] + dn[i] + 2.0 * u[i])
            VE[i, 8 * t : 8 * t + 8, :] = edge(v)
            vz = (1.0 / 64.0) * (pltpu.roll(v, 1, 1) + 2.0 * v + pltpu.roll(v, 127, 1))
            VHE[i, 8 * t : 8 * t + 8, :] = edge(vz)
    for p in range(12):
        for t in range(2):
            a = TZ[p, 8 * t : 8 * t + 8, :] + 2.0 * TZ[p, 8 * t + 1 : 8 * t + 9, :] + TZ[p, 8 * t + 2 : 8 * t + 10, :]
            ZE[p, 8 * t : 8 * t + 8, :] = edge(xsum(a))

    first_lane, last_lane = lane == 0, lane == 127

    def zshift(a, e):
        p0, p1 = pltpu.roll(a[0], 1, 1), pltpu.roll(a[1], 1, 1)
        n0, n1 = pltpu.roll(a[0], 127, 1), pltpu.roll(a[1], 127, 1)
        prev = (jnp.where(first_lane, e, p0), jnp.where(first_lane, p0, p1))
        nxt = (jnp.where(last_lane, n1, n0), jnp.where(last_lane, e, n1))
        return prev, nxt

    def stage_a(X, _):
        turn = 127 - 6 * X
        for t in range(3):
            r0 = BASE - 1 + 8 * t
            u = [[U[i, zt, X, r0 : r0 + 8, :] for zt in range(2)] for i in range(3)]
            zs = [zshift(u[i], pltpu.roll(UE[i, 8 * t : 8 * t + 8, :], turn, 1)) for i in range(3)]
            for zt in range(2):
                d = []
                for i in range(3):
                    ddx = U[i, zt, X + 1, r0 : r0 + 8, :] - U[i, zt, X - 1, r0 : r0 + 8, :]
                    ddy = U[i, zt, X, r0 + 1 : r0 + 9, :] - U[i, zt, X, r0 - 1 : r0 + 7, :]
                    d.append([ddx, ddy, zs[i][1][zt] - zs[i][0][zt]])
                m = [U[3 + j, zt, X, r0 : r0 + 8, :] for j in range(3)]
                s, mag = strain_of(d, m)
                for p, (a, b) in enumerate(PAIRS):
                    T[p, zt, 8 * t : 8 * t + 8, :] = u[a][zt] * u[b][zt]
                    T[6 + p, zt, 8 * t : 8 * t + 8, :] = (0.5 if a == b else 0.25) * mag * s[p]
                MB[X, zt, 8 * t : 8 * t + 8, :] = mag
        for p in range(12):
            for zt in range(2):
                for t in range(2):
                    r = 8 * t
                    YF[p, zt, X, r : r + 8, :] = (
                        T[p, zt, r : r + 8, :] + 2.0 * T[p, zt, r + 1 : r + 9, :] + T[p, zt, r + 2 : r + 10, :])
        return 0


    def stage_y(X, _):
        for i in range(3):
            for zt in range(2):
                for t in range(3):
                    r = BASE - 1 + 8 * t
                    YV[i, zt, X, 8 * t : 8 * t + 8, :] = (
                        U[i, zt, X, r - 1 : r + 7, :] + 2.0 * U[i, zt, X, r : r + 8, :] + U[i, zt, X, r + 1 : r + 9, :])
        return 0


    def stage_v(X, _):
        turn = 127 - 6 * X
        x_in = jnp.logical_and(jnp.logical_or(X >= 2, gx > 0), jnp.logical_or(X < nx + 2, gx < ngx - 1))
        for t in range(3):
            rr_ = row + 8 * t
            y_in = jnp.logical_and(rr_ >= jnp.where(gy > 0, 0, 1), rr_ < jnp.where(gy < ngy - 1, ny + 2, ny + 1))
            inside = jnp.logical_and(y_in, x_in)
            for i in range(3):
                a = [YV[i, zt, X - 1, 8 * t : 8 * t + 8, :] + 2.0 * YV[i, zt, X, 8 * t : 8 * t + 8, :]
                     + YV[i, zt, X + 1, 8 * t : 8 * t + 8, :] for zt in range(2)]
                prev, nxt = zshift(a, pltpu.roll(VE[i, 8 * t : 8 * t + 8, :], turn, 1))
                for zt in range(2):
                    v = (1.0 / 64.0) * (prev[zt] + 2.0 * a[zt] + nxt[zt])
                    VH[i, zt, X, 8 * t : 8 * t + 8, :] = jnp.where(inside, v, 0.0)
        return 0


    def stage_c(X, _):
        turn = 127 - 6 * X
        for t in range(2):
            r = 8 * t
            v = [[VH[i, zt, X, r + 1 : r + 9, :] for zt in range(2)] for i in range(3)]
            zs = [zshift(v[i], pltpu.roll(VHE[i, r + 1 : r + 9, :], turn, 1)) for i in range(3)]
            fl = []
            for p in range(12):
                a = [YF[p, zt, X - 1, r : r + 8, :] + 2.0 * YF[p, zt, X, r : r + 8, :]
                     + YF[p, zt, X + 1, r : r + 8, :] for zt in range(2)]
                prev, nxt = zshift(a, pltpu.roll(ZE[p, r : r + 8, :], turn, 1))
                fl.append([(1.0 / 64.0) * (prev[zt] + 2.0 * a[zt] + nxt[zt]) for zt in range(2)])
            num = den = None
            for zt in range(2):
                d = []
                for i in range(3):
                    ddx = VH[i, zt, X + 1, r + 1 : r + 9, :] - VH[i, zt, X - 1, r + 1 : r + 9, :]
                    ddy = VH[i, zt, X, r + 2 : r + 10, :] - VH[i, zt, X, r : r + 8, :]
                    d.append([ddx, ddy, zs[i][1][zt] - zs[i][0][zt]])
                m = [U[3 + j, zt, X, BASE + r : BASE + r + 8, :] for j in range(3)]
                s, mag = strain_of(d, m)
                delta = jnp.exp2((-2.0 / 3.0) * jnp.log2(m[0] * m[1] * m[2]))
                nn = dd = None
                for p, (a, b) in enumerate(PAIRS):
                    w = 1.0 if a == b else 2.0
                    leo = fl[p][zt] - v[a][zt] * v[b][zt]
                    q = fl[6 + p][zt] - (2.0 if a == b else 1.0) * mag * s[p]
                    wq = q if a == b else w * q
                    n_, d_ = wq * leo, wq * q
                    nn = n_ if nn is None else nn + n_
                    dd = d_ if dd is None else dd + d_
                d2 = 2.0 * delta
                n_, d_ = d2 * nn, d2 * d2 * dd
                num = n_ if num is None else num + n_
                den = d_ if den is None else den + d_
                DM[X - 2, zt, r : r + 8, :] = delta * MB[X, zt, r + 1 : r + 9, :]
            NP[0, X - 2, r : r + 8, :] = num
            NP[1, X - 2, r : r + 8, :] = den
        return 0

    def line_sums(acc, planes):
        for x in planes:
            for t in range(2):
                for k in range(2):
                    part = jnp.sum(NP[k, x, 8 * t : 8 * t + 8, :], axis=1, keepdims=True)
                    acc = jnp.where(lane == x + nx * t + 2 * nx * k, part, acc)
        return acc

    got(2)
    got(3)

    for s in range(2):
        for f in range(6):
            for k in range(2):
                if f >= 3 and k == s:
                    continue
                y = (ny + k) if s else k - 2
                slab = 2 * f + k if f < 3 else 3 + f
                for zt in range(2):
                    U[f, zt, pl.ds(2, nx), BASE + y, :] = RY[s, slab, zt, :, :]
    lax.fori_loop(3, nx + 1, stage_a, 0, unroll=UA)
    lax.fori_loop(2, nx + 2, stage_y, 0, unroll=UY)
    lax.fori_loop(3, nx + 1, stage_v, 0, unroll=UV)
    lax.fori_loop(4, nx, stage_c, 0, unroll=UC)

    sums = line_sums(z8, range(2, nx - 2))

    for n in range(4, 12):
        got(n)
    for sx in range(2):
        for sy in range(2):
            for r, zt, f, kx, ky in corner_rows(1 - sx, 1 - sy):
                X, yr = (nx + 2 if sx else 0) + kx, (ny if sy else -2) + ky + BASE
                U[f, zt, X, yr : yr + 1, :] = RC[2 * sx + sy, r : r + 1, :]

    def ends(a, stage):
        lax.fori_loop(0, 4, lambda k, c: stage(jnp.where(k < 2, a + k, nx - a + k), c), 0, unroll=UE4)

    ends(1, stage_a)
    ends(0, stage_y)
    ends(1, stage_v)
    ends(2, stage_c)
    LN[gz] = line_sums(sums, (0, 1, nx - 2, nx - 1))

    outs = []
    for zt in range(2):
        cp = pltpu.make_async_copy(DM.at[:, zt], dm_out.at[:, :, pl.ds(128 * zt, 128)], lsem.at[4 + zt])
        cp.start()
        outs.append(cp)

    cps = []
    for k in range(1, ngz):
        cp = pltpu.make_async_remote_copy(
            src_ref=LN.at[gz], dst_ref=LN.at[gz], send_sem=ssem.at[40 + k], recv_sem=rsem.at[40 + gz],
            device_id={"gz": lax.rem(gz + k, ngz)}, device_id_type=MESH)
        cp.start()
        cps.append(cp)
    for k in range(1, ngz):
        src = lax.rem(gz + k, ngz)
        pltpu.make_async_remote_copy(
            src_ref=LN.at[gz], dst_ref=LN.at[src], send_sem=ssem.at[40 + k], recv_sem=rsem.at[40 + src],
            device_id={"gz": src}, device_id_type=MESH).wait_recv()
    tot = LN[0]
    for k in range(1, ngz):
        tot = tot + LN[k]
    tot = tot * (1.0 / (nz * ngz))
    den = pltpu.roll(tot, 128 - 2 * nx, 1)
    line = tot / (den + 1e-06)
    valid = lane < 2 * nx
    peak = jnp.max(jnp.where(valid, line, -jnp.inf), axis=0, keepdims=True)
    peak = jnp.max(peak, axis=1, keepdims=True)

    RX[me_c] = jnp.broadcast_to(peak, (1, 128))
    for k in range(1, nxc):
        c, dev = xc_dev(k)
        cp = pltpu.make_async_remote_copy(
            src_ref=RX.at[me_c], dst_ref=RX.at[me_c], send_sem=ssem.at[44 + k], recv_sem=rsem.at[44 + me_c],
            device_id=dev, device_id_type=MESH)
        cp.start()
        cps.append(cp)
    for k in range(1, nxc):
        c, dev = xc_dev(k)
        pltpu.make_async_remote_copy(
            src_ref=RX.at[me_c], dst_ref=RX.at[c], send_sem=ssem.at[44 + k], recv_sem=rsem.at[44 + c],
            device_id=dev, device_id_type=MESH).wait_recv()
    peak = RX[0]
    for k in range(1, nxc):
        peak = jnp.maximum(peak, RX[k])
    RZ[xz] = peak
    for k in range(1, nzc):
        c, dev = z_dev(k)
        cp = pltpu.make_async_remote_copy(
            src_ref=RZ.at[xz], dst_ref=RZ.at[xz], send_sem=ssem.at[52 + k], recv_sem=rsem.at[52 + xz],
            device_id=dev, device_id_type=MESH)
        cp.start()
        cps.append(cp)
    for k in range(1, nzc):
        c, dev = z_dev(k)
        pltpu.make_async_remote_copy(
            src_ref=RZ.at[xz], dst_ref=RZ.at[c], send_sem=ssem.at[52 + k], recv_sem=rsem.at[52 + c],
            device_id=dev, device_id_type=MESH).wait_recv()
    peak = RZ[0]
    for k in range(1, nzc):
        peak = jnp.maximum(peak, RZ[k])

    half_out[...] = 0.5 * peak
    lt = line.T
    for t in range(2):
        line_out[:, 8 * t : 8 * t + 8] = lt[nx * t : nx * t + nx, :]
    for cp in outs:
        cp.wait()

    for cp in cps:
        cp.wait_send()
    for cp, cond in waits_send:
        if cond is None:
            cp.wait_send()
        else:
            pl.when(cond)(cp.wait_send)


def solution(mesh):
    sizes = tuple(mesh.shape[a] for a in ("gx", "gy", "gz"))
    ngx, ngy, ngz = sizes

    def per_device(velocity, metric):
        _, nx, ny, nz = velocity.shape
        vm = lambda *s: pltpu.VMEM(s, F32)
        dm, line, half = pl.pallas_call(
            functools.partial(kernel, sizes),
            out_shape=(vm(nx, ny, nz), vm(nx, ny), vm(1, 128)),
            in_specs=[pl.BlockSpec(memory_space=pl.ANY)] * 2,
            out_specs=(pl.BlockSpec(memory_space=pl.ANY),) + (pl.BlockSpec(memory_space=pltpu.VMEM),) * 2,
            scratch_shapes=[
                vm(6, 2, nx + 4, PITCH, 128),
                vm(6, 16, 128),
                vm(2, 9, 2, nx, 128),
                vm(2, 9, 2, nx, 128),
                vm(4, 24, 128),
                vm(4, 24, 128),
                vm(2, 6, 16, 128),
                vm(6, 32, 128),
                vm(2, 8, 128),
                vm(3, 2, 8, 128),
                vm(2, 16, 128),
                vm(3, 2, 16, 128),
                vm(4, 2, 1, 128),
                vm(3, 4, 2, 1, 128),
                vm(4, 8, 128),
                vm(2, 16, 128),
                vm(12, 24, 128),
                vm(3, 24, 128),
                vm(12, 16, 128),
                vm(3, 24, 128),
                vm(3, 24, 128),
                vm(12, 2, 24, 128),
                vm(12, 2, nx + 4, 16, 128),
                vm(3, 2, nx + 4, 24, 128),
                vm(3, 2, nx + 4, 24, 128),
                vm(nx + 4, 2, 24, 128),
                vm(nx, 2, 16, 128),
                vm(2, nx, 16, 128),
                vm(ngz, 8, 128),
                vm(2 * ngy, 1, 128),
                vm(ngx // 2, 1, 128),
                pltpu.SemaphoreType.DMA((6,)),
                pltpu.SemaphoreType.DMA((60,)),
                pltpu.SemaphoreType.DMA((60,)),
            ],
            compiler_params=pltpu.CompilerParams(collective_id=0, has_side_effects=True),
        )(velocity, metric)
        coefficient = jnp.minimum(line, half[0, 0])
        return coefficient[:, :, None] * dm, coefficient

    return jax.shard_map(
        per_device,
        mesh=mesh,
        in_specs=(P(None, "gx", "gy", "gz"), P(None, "gx", "gy", "gz")),
        out_specs=(P("gx", "gy", "gz"), P("gx", "gy")),
        check_vma=False,
    )
```

```python
import functools
import jax
import jax.numpy as jnp
from jax import lax
from jax.experimental import pallas as pl
from jax.experimental.pallas import tpu as pltpu
from jax.sharding import PartitionSpec as P

PAIRS = ((0, 0), (1, 1), (2, 2), (0, 1), (0, 2), (1, 2))
F32 = jnp.float32
MESH = pl.DeviceIdType.MESH
PITCH = 32
BASE = 8
UA, UY, UV, UC, UE4 = 2, 4, 7, 4, 4


def strain_of(diffs, m):
    g = [[m[j] * diffs[i][j] for j in range(3)] for i in range(3)]
    s = [g[a][a] if a == b else g[a][b] + g[b][a] for a, b in PAIRS]
    diag = s[0] * s[0] + s[1] * s[1] + s[2] * s[2]
    off = s[3] * s[3] + s[4] * s[4] + s[5] * s[5]
    return s, jnp.sqrt(0.5 * diag + 0.25 * off)


def kernel(sizes, vel, met, dm_out, line_out, half_out, U, O6, SY, RY, SC, RC, RO, ZG, SZX, RZX, SZY, RZY,
           SZC, RZC, ZC, SZG, TZ, UE, ZE, VE, VHE, T, YF, YV, VH, MB, DM, NP, LN, RX, lsem, ssem, rsem):
    ngx, ngy, ngz = sizes
    nx = vel.shape[1]
    ny = vel.shape[2]
    nz = vel.shape[3]
    gx, gy, gz = lax.axis_index("gx"), lax.axis_index("gy"), lax.axis_index("gz")
    has = {("x", 0): gx > 0, ("x", 1): gx < ngx - 1, ("y", 0): gy > 0, ("y", 1): gy < ngy - 1}

    ins = []
    for zt in range(2):
        for k, ref in enumerate((vel, met)):
            cp = pltpu.make_async_copy(
                ref.at[:, :, :, pl.ds(128 * zt, 128)],
                U.at[pl.ds(3 * k, 3), zt, pl.ds(2, nx), pl.ds(BASE, ny), :],
                lsem.at[2 * zt + k],
            )
            cp.start()
            ins.append(cp)

    bar = pltpu.get_barrier_semaphore()

    def greet(dev):
        pl.semaphore_signal(bar, inc=1, device_id=dev, device_id_type=MESH)

    def dx(s):
        return gx + (1 if s else -1)

    def dy(s):
        return gy + (1 if s else -1)

    def gz_at(d):
        return lax.rem(gz + d + ngz, ngz)

    both = {(sx, sy): jnp.logical_and(has["x", sx], has["y", sy]) for sx in range(2) for sy in range(2)}
    for d in (-1, 1):
        greet({"gz": gz_at(d)})
    for s in range(2):
        @pl.when(has["y", s])
        def _():
            for d in (-1, 0, 1):
                greet({"gy": dy(s), "gz": gz_at(d)})

        @pl.when(has["x", s])
        def _():
            for d in (-1, 0, 1):
                greet({"gx": dx(s), "gz": gz_at(d)})

        for q in range(2):
            @pl.when(both[s, q])
            def _():
                for d in (-1, 0, 1):
                    greet({"gx": dx(s), "gy": dy(q), "gz": gz_at(d)})

    core, xhi, nhi = lax.rem(gy, 2), lax.div(gy, 2), ngy // 2
    n1, n2 = 2 * ngz, ngx * nhi
    me1, me2 = core * ngz + gz, gx * nhi + xhi

    def dev1(k):
        c = lax.rem(me1 + k, n1)
        return c, {"gy": 2 * xhi + lax.div(c, ngz), "gz": lax.rem(c, ngz)}

    def dev2(k):
        c = lax.rem(me2 + k, n2)
        return c, {"gx": lax.div(c, nhi), "gy": 2 * lax.rem(c, nhi) + core}

    for k in range(1, n1):
        greet(dev1(k)[1])
    for k in range(1, n2):
        greet(dev2(k)[1])
    ex = has["x", 0].astype(jnp.int32) + has["x", 1].astype(jnp.int32)
    ey = has["y", 0].astype(jnp.int32) + has["y", 1].astype(jnp.int32)
    partners = 3 * (1 + ex) * (1 + ey) - 1 + n1 - 1 + n2 - 1

    z8 = jnp.zeros((8, 128), F32)
    for s in range(2):
        @pl.when(jnp.logical_not(has["x", s]))
        def _():
            for f in range(6):
                for zt in range(2):
                    for X in ((nx + 2, nx + 3) if s else (0, 1)):
                        for r in range(0, ny, 8):
                            U[f, zt, X, BASE + r : BASE + r + 8, :] = z8
            for d in range(3):
                RZX[d, s] = jnp.zeros(RZX.shape[2:], F32)

        @pl.when(jnp.logical_not(has["y", s]))
        def _():
            RY[s] = jnp.zeros(RY.shape[1:], F32)
            for d in range(3):
                RZY[d, s] = jnp.zeros(RZY.shape[2:], F32)

        for q in range(2):
            @pl.when(jnp.logical_not(both[s, q]))
            def _():
                RC[2 * s + q] = jnp.zeros(RC.shape[1:], F32)
                for d in range(3):
                    RZC[d, 2 * s + q] = jnp.zeros(RZC.shape[2:], F32)

    for cp in ins:
        cp.wait()
    for s in range(2):
        for f in range(6):
            for k in range(2):
                if f >= 3 and k != s:
                    continue
                y = (ny - 2 + k) if s else k
                slab = 2 * f + k if f < 3 else 3 + f
                for zt in range(2):
                    SY[s, slab, zt, :, :] = U[f, zt, pl.ds(2, nx), BASE + y, :]

    pl.semaphore_wait(bar, partners)

    waits_send, waits_recv = [], {}

    def put(n, src, dst, dev, send_if=None, recv_if=None):
        cp = pltpu.make_async_remote_copy(
            src_ref=src, dst_ref=dst, send_sem=ssem.at[n], recv_sem=rsem.at[n],
            device_id=dev, device_id_type=MESH)
        if send_if is None:
            cp.start()
        else:
            pl.when(send_if)(cp.start)
        waits_send.append((cp, send_if))
        waits_recv[n] = (cp, recv_if)

    def got(n):
        cp, cond = waits_recv[n]
        if cond is None:
            cp.wait_recv()
        else:
            pl.when(cond)(cp.wait_recv)

    for s in range(2):
        put(2 + s, SY.at[s], RY.at[1 - s], {"gy": dy(s)}, has["y", s], has["y", 1 - s])

    lane = lax.broadcasted_iota(jnp.int32, (8, 128), 1)
    lx = lax.shift_right_logical(lane * 43, 8)
    lc = lane - 6 * lx
    row = lax.broadcasted_iota(jnp.int32, (8, 128), 0)
    half = lane < 64
    for f in range(6):
        for t in range(2):
            acc = z8
            rows = slice(BASE + 8 * t, BASE + 8 * t + 8)
            for X in range(2, nx + 2):
                a = jnp.where(half, U[f, 0, X, rows, :], U[f, 1, X, rows, :])
                acc = jnp.where(lx == X, pltpu.roll(a, (6 * X + 2) % 128, 1), acc)
            O6[f, 8 * t : 8 * t + 8, :] = acc

    def x_at(f, t):
        return 54 * t + (12 * f if f < 3 else 18 + 6 * f)

    def x_lanes(lanes, at, f):
        return jnp.logical_and(lanes >= at, lanes < at + (12 if f < 3 else 6))

    for s in range(2):
        acc = z8
        for t in range(2):
            for f in range(6):
                first = 6 * ((nx + (f >= 3)) if s else 2)
                part = pltpu.roll(O6[f, 8 * t : 8 * t + 8, :], (x_at(f, t) - first) % 128, 1)
                acc = jnp.where(x_lanes(lane, x_at(f, t), f), part, acc)
        SZX[s] = acc
        for sy in range(2):
            for k in range(2):
                SZC[2 * s + sy, k] = acc[6 + k : 7 + k] if sy else acc[k : k + 1]
        y = ny - 2 if s else 0
        for f in range(6):
            SZY[s, 2 * f : 2 * f + 2, :] = O6[f, y : y + 2, :]
        SZY[s, 12:16, :] = z8[0:4]

    def corner_rows(sx, sy):
        rows = [(f, kx, ky) for f in range(6) for kx in range(2) for ky in range(2)
                if (kx == sx and ky == sy) or (f < 3 and (kx == sx or ky == sy))]
        return [(12 * zt + r, zt, *q) for zt in range(2) for r, q in enumerate(rows)]

    for sx in range(2):
        for sy in range(2):
            for r, zt, f, kx, ky in corner_rows(sx, sy):
                X, yr = (nx if sx else 2) + kx, (ny - 2 if sy else 0) + ky + BASE
                SC[2 * sx + sy, r : r + 1, :] = U[f, zt, X, yr : yr + 1, :]

    for s in range(2):
        put(s, O6, RO.at[1 - s], {"gz": gz_at(1 if s else -1)})
    for i, d in enumerate((-1, 0, 1)):
        o = 2 - i
        for s in range(2):
            put(12 + 2 * i + s, SZY.at[s], RZY.at[o, 1 - s], {"gy": dy(s), "gz": gz_at(d)},
                has["y", s], has["y", 1 - s])
            put(18 + 2 * i + s, SZX.at[s], RZX.at[o, 1 - s], {"gx": dx(s), "gz": gz_at(d)},
                has["x", s], has["x", 1 - s])
        for sx in range(2):
            for sy in range(2):
                put(24 + 4 * i + 2 * sx + sy, SZC.at[2 * sx + sy],
                    RZC.at[o, 2 * (1 - sx) + 1 - sy],
                    {"gx": dx(sx), "gy": dy(sy), "gz": gz_at(d)},
                    both[sx, sy], both[1 - sx, 1 - sy])
    for sx in range(2):
        for sy in range(2):
            put(8 + 2 * sx + sy, SC.at[2 * sx + sy], RC.at[2 * (1 - sx) + 1 - sy],
                {"gx": dx(sx), "gy": dy(sy)}, both[sx, sy], both[1 - sx, 1 - sy])
    def comb(left, own, right):
        return jnp.where(lc < 2, left, jnp.where(lc == 2, own, pltpu.roll(jnp.where(lc == 1, own, right), 2, 1)))

    got(0)
    got(1)
    for n in (12,13,14,15,16,17):
        got(n)
    rr = pl.ds(BASE, ny)
    for s in range(2):
        far, near = (nx, nx + 1) if s else (3, 2)
        gfar, gnear = (0, 1) if s else (nx + 3, nx + 2)
        put(4 + s, U.at[:, :, near, rr, :], U.at[:, :, gnear, rr, :], {"gx": dx(s)},
            has["x", s], has["x", 1 - s])
        put(6 + s, U.at[pl.ds(0, 3), :, far, rr, :], U.at[pl.ds(0, 3), :, gfar, rr, :],
            {"gx": dx(s)}, has["x", s], has["x", 1 - s])
    for n in range(18, 36):
        got(n)
    zx = [comb(RZX[0, s], RZX[1, s], RZX[2, s]) for s in range(2)]
    for s in range(2):
        for t in range(2):
            rows = slice(8 * t, 8 * t + 8)
            SZG[s, rows, :] = comb(RZY[0, s, rows, :], RZY[1, s, rows, :], RZY[2, s, rows, :])
    lane1 = lc[0:1]
    for c in range(4):
        ZC[c] = z8
        for k in range(2):
            left, own, right = (RZC[d, c, k] for d in range(3))
            ZC[c, k : k + 1, :] = jnp.where(lane1 < 2, left, jnp.where(
                lane1 == 2, own, pltpu.roll(jnp.where(lane1 == 1, own, right), 2, 1)))

    def x_place(sx, f):
        return 6 * (nx + 2) if sx else (0 if f < 3 else 6)

    for f in range(6):
        ZG[f, 0:8, :] = z8
        ZG[f, 24:32, :] = z8
        for t in range(2):
            rows = slice(8 * t, 8 * t + 8)
            z = comb(RO[0, f, rows, :], O6[f, rows, :], RO[1, f, rows, :])
            for sx in range(2):
                at = x_place(sx, f)
                part = pltpu.roll(zx[sx], (at - x_at(f, t)) % 128, 1)
                z = jnp.where(x_lanes(lane, at, f), part, z)
            ZG[f, BASE + 8 * t : BASE + 8 * t + 8, :] = z
        for sy in range(2):
            yr = BASE + (ny if sy else -2)
            z = SZG[sy, 2 * f : 2 * f + 2, :]
            for sx in range(2):
                at = x_place(sx, f)
                part = pltpu.roll(ZC[2 * sx + sy], (at - x_at(f, 1 - sy)) % 128, 1)[0:2]
                z = jnp.where(x_lanes(lane[0:2], at, f), part, z)
            ZG[f, yr : yr + 2, :] = z

    def edge(a):
        return jnp.where(lc == 0, pltpu.roll(a, 124, 1), a)

    def xsum(a):
        return pltpu.roll(a, 6, 1) + 2.0 * a + pltpu.roll(a, 122, 1)

    xd = lambda a: pltpu.roll(a, 122, 1) - pltpu.roll(a, 6, 1)
    zd = lambda a: pltpu.roll(a, 127, 1) - pltpu.roll(a, 1, 1)
    for t in range(3):
        r0 = BASE - 1 + 8 * t
        at = lambda f, d: ZG[f, r0 + d : r0 + d + 8, :]
        u = [at(i, 0) for i in range(3)]
        up = [at(i, 1) for i in range(3)]
        dn = [at(i, -1) for i in range(3)]
        m = [at(3 + j, 0) for j in range(3)]
        d = [[xd(u[i]), up[i] - dn[i], zd(u[i])] for i in range(3)]
        s, mag = strain_of(d, m)
        for p, (a, b) in enumerate(PAIRS):
            TZ[p, 8 * t : 8 * t + 8, :] = u[a] * u[b]
            TZ[6 + p, 8 * t : 8 * t + 8, :] = (0.5 if a == b else 0.25) * mag * s[p]
        for i in range(3):
            UE[i, 8 * t : 8 * t + 8, :] = edge(u[i])
            v = xsum(up[i] + dn[i] + 2.0 * u[i])
            VE[i, 8 * t : 8 * t + 8, :] = edge(v)
            vz = (1.0 / 64.0) * (pltpu.roll(v, 1, 1) + 2.0 * v + pltpu.roll(v, 127, 1))
            VHE[i, 8 * t : 8 * t + 8, :] = edge(vz)
    for p in range(12):
        for t in range(2):
            a = TZ[p, 8 * t : 8 * t + 8, :] + 2.0 * TZ[p, 8 * t + 1 : 8 * t + 9, :] + TZ[p, 8 * t + 2 : 8 * t + 10, :]
            ZE[p, 8 * t : 8 * t + 8, :] = edge(xsum(a))

    first_lane, last_lane = lane == 0, lane == 127

    def zshift(a, e):
        p0, p1 = pltpu.roll(a[0], 1, 1), pltpu.roll(a[1], 1, 1)
        n0, n1 = pltpu.roll(a[0], 127, 1), pltpu.roll(a[1], 127, 1)
        prev = (jnp.where(first_lane, e, p0), jnp.where(first_lane, p0, p1))
        nxt = (jnp.where(last_lane, n1, n0), jnp.where(last_lane, e, n1))
        return prev, nxt

    def stage_a(X, _):
        turn = 127 - 6 * X
        for t in range(3):
            r0 = BASE - 1 + 8 * t
            u = [[U[i, zt, X, r0 : r0 + 8, :] for zt in range(2)] for i in range(3)]
            zs = [zshift(u[i], pltpu.roll(UE[i, 8 * t : 8 * t + 8, :], turn, 1)) for i in range(3)]
            for zt in range(2):
                d = []
                for i in range(3):
                    ddx = U[i, zt, X + 1, r0 : r0 + 8, :] - U[i, zt, X - 1, r0 : r0 + 8, :]
                    ddy = U[i, zt, X, r0 + 1 : r0 + 9, :] - U[i, zt, X, r0 - 1 : r0 + 7, :]
                    d.append([ddx, ddy, zs[i][1][zt] - zs[i][0][zt]])
                m = [U[3 + j, zt, X, r0 : r0 + 8, :] for j in range(3)]
                s, mag = strain_of(d, m)
                for p, (a, b) in enumerate(PAIRS):
                    T[p, zt, 8 * t : 8 * t + 8, :] = u[a][zt] * u[b][zt]
                    T[6 + p, zt, 8 * t : 8 * t + 8, :] = (0.5 if a == b else 0.25) * mag * s[p]
                MB[X, zt, 8 * t : 8 * t + 8, :] = mag
        for p in range(12):
            for zt in range(2):
                for t in range(2):
                    r = 8 * t
                    YF[p, zt, X, r : r + 8, :] = (
                        T[p, zt, r : r + 8, :] + 2.0 * T[p, zt, r + 1 : r + 9, :] + T[p, zt, r + 2 : r + 10, :])
        return 0


    def stage_y(X, _):
        for i in range(3):
            for zt in range(2):
                for t in range(3):
                    r = BASE - 1 + 8 * t
                    YV[i, zt, X, 8 * t : 8 * t + 8, :] = (
                        U[i, zt, X, r - 1 : r + 7, :] + 2.0 * U[i, zt, X, r : r + 8, :] + U[i, zt, X, r + 1 : r + 9, :])
        return 0


    def stage_v(X, _):
        turn = 127 - 6 * X
        x_in = jnp.logical_and(jnp.logical_or(X >= 2, gx > 0), jnp.logical_or(X < nx + 2, gx < ngx - 1))
        for t in range(3):
            rr_ = row + 8 * t
            y_in = jnp.logical_and(rr_ >= jnp.where(gy > 0, 0, 1), rr_ < jnp.where(gy < ngy - 1, ny + 2, ny + 1))
            inside = jnp.logical_and(y_in, x_in)
            for i in range(3):
                a = [YV[i, zt, X - 1, 8 * t : 8 * t + 8, :] + 2.0 * YV[i, zt, X, 8 * t : 8 * t + 8, :]
                     + YV[i, zt, X + 1, 8 * t : 8 * t + 8, :] for zt in range(2)]
                prev, nxt = zshift(a, pltpu.roll(VE[i, 8 * t : 8 * t + 8, :], turn, 1))
                for zt in range(2):
                    v = (1.0 / 64.0) * (prev[zt] + 2.0 * a[zt] + nxt[zt])
                    VH[i, zt, X, 8 * t : 8 * t + 8, :] = jnp.where(inside, v, 0.0)
        return 0


    def stage_c(X, _):
        turn = 127 - 6 * X
        for t in range(2):
            r = 8 * t
            v = [[VH[i, zt, X, r + 1 : r + 9, :] for zt in range(2)] for i in range(3)]
            zs = [zshift(v[i], pltpu.roll(VHE[i, r + 1 : r + 9, :], turn, 1)) for i in range(3)]
            fl = []
            for p in range(12):
                a = [YF[p, zt, X - 1, r : r + 8, :] + 2.0 * YF[p, zt, X, r : r + 8, :]
                     + YF[p, zt, X + 1, r : r + 8, :] for zt in range(2)]
                prev, nxt = zshift(a, pltpu.roll(ZE[p, r : r + 8, :], turn, 1))
                fl.append([(1.0 / 64.0) * (prev[zt] + 2.0 * a[zt] + nxt[zt]) for zt in range(2)])
            num = den = None
            for zt in range(2):
                d = []
                for i in range(3):
                    ddx = VH[i, zt, X + 1, r + 1 : r + 9, :] - VH[i, zt, X - 1, r + 1 : r + 9, :]
                    ddy = VH[i, zt, X, r + 2 : r + 10, :] - VH[i, zt, X, r : r + 8, :]
                    d.append([ddx, ddy, zs[i][1][zt] - zs[i][0][zt]])
                m = [U[3 + j, zt, X, BASE + r : BASE + r + 8, :] for j in range(3)]
                s, mag = strain_of(d, m)
                delta = jnp.exp2((-2.0 / 3.0) * jnp.log2(m[0] * m[1] * m[2]))
                nn = dd = None
                for p, (a, b) in enumerate(PAIRS):
                    w = 1.0 if a == b else 2.0
                    leo = fl[p][zt] - v[a][zt] * v[b][zt]
                    q = fl[6 + p][zt] - (2.0 if a == b else 1.0) * mag * s[p]
                    wq = q if a == b else w * q
                    n_, d_ = wq * leo, wq * q
                    nn = n_ if nn is None else nn + n_
                    dd = d_ if dd is None else dd + d_
                d2 = 2.0 * delta
                n_, d_ = d2 * nn, d2 * d2 * dd
                num = n_ if num is None else num + n_
                den = d_ if den is None else den + d_
                DM[X - 2, zt, r : r + 8, :] = delta * MB[X, zt, r + 1 : r + 9, :]
            NP[0, X - 2, r : r + 8, :] = num
            NP[1, X - 2, r : r + 8, :] = den
        return 0

    def line_sums(acc, planes):
        for x in planes:
            for t in range(2):
                for k in range(2):
                    part = jnp.sum(NP[k, x, 8 * t : 8 * t + 8, :], axis=1, keepdims=True)
                    acc = jnp.where(lane == x + nx * t + 2 * nx * k, part, acc)
        return acc

    got(2)
    got(3)

    for s in range(2):
        for f in range(6):
            for k in range(2):
                if f >= 3 and k == s:
                    continue
                y = (ny + k) if s else k - 2
                slab = 2 * f + k if f < 3 else 3 + f
                for zt in range(2):
                    U[f, zt, pl.ds(2, nx), BASE + y, :] = RY[s, slab, zt, :, :]
    lax.fori_loop(3, nx + 1, stage_a, 0, unroll=UA)
    lax.fori_loop(2, nx + 2, stage_y, 0, unroll=UY)
    lax.fori_loop(3, nx + 1, stage_v, 0, unroll=UV)
    lax.fori_loop(4, nx, stage_c, 0, unroll=UC)

    sums = line_sums(z8, range(2, nx - 2))

    for n in range(4, 12):
        got(n)
    for sx in range(2):
        for sy in range(2):
            for r, zt, f, kx, ky in corner_rows(1 - sx, 1 - sy):
                X, yr = (nx + 2 if sx else 0) + kx, (ny if sy else -2) + ky + BASE
                U[f, zt, X, yr : yr + 1, :] = RC[2 * sx + sy, r : r + 1, :]

    def ends(a, stage):
        lax.fori_loop(0, 4, lambda k, c: stage(jnp.where(k < 2, a + k, nx - a + k), c), 0, unroll=UE4)

    ends(1, stage_a)
    ends(0, stage_y)
    ends(1, stage_v)
    ends(2, stage_c)
    LN[me1] = line_sums(sums, (0, 1, nx - 2, nx - 1))

    outs = []
    for zt in range(2):
        cp = pltpu.make_async_copy(DM.at[:, zt], dm_out.at[:, :, pl.ds(128 * zt, 128)], lsem.at[4 + zt])
        cp.start()
        outs.append(cp)

    cps = []

    def spread(ref, me, n, dev, at):
        def copy(k, c):
            return pltpu.make_async_remote_copy(
                src_ref=ref.at[me], dst_ref=ref.at[c], send_sem=ssem.at[at + k], recv_sem=rsem.at[at + c],
                device_id=dev(k)[1], device_id_type=MESH)

        for k in range(1, n):
            cp = copy(k, me)
            cp.start()
            cps.append(cp)
        for k in range(1, n):
            copy(k, dev(k)[0]).wait_recv()

    spread(LN, me1, n1, dev1, 36)

    def line_of(q):
        tot = LN[q * ngz]
        for k in range(1, ngz):
            tot = tot + LN[q * ngz + k]
        tot = tot * (1.0 / (nz * ngz))
        return tot / (pltpu.roll(tot, 128 - 2 * nx, 1) + 1e-06)

    peak = jnp.where(lane < 2 * nx, jnp.maximum(line_of(0), line_of(1)), -jnp.inf)
    peak = jnp.max(jnp.max(peak, axis=0, keepdims=True), axis=1, keepdims=True)

    RX[me2] = jnp.broadcast_to(peak, (1, 128))
    spread(RX, me2, n2, dev2, 36 + n1)
    peak = RX[0]
    for k in range(1, n2):
        peak = jnp.maximum(peak, RX[k])
    line = line_of(core)

    half_out[...] = 0.5 * peak
    lt = line.T
    for t in range(2):
        line_out[:, 8 * t : 8 * t + 8] = lt[nx * t : nx * t + nx, :]
    for cp in outs:
        cp.wait()

    for cp in cps:
        cp.wait_send()
    for cp, cond in waits_send:
        if cond is None:
            cp.wait_send()
        else:
            pl.when(cond)(cp.wait_send)


def solution(mesh):
    sizes = tuple(mesh.shape[a] for a in ("gx", "gy", "gz"))
    ngx, ngy, ngz = sizes

    def per_device(velocity, metric):
        _, nx, ny, nz = velocity.shape
        vm = lambda *s: pltpu.VMEM(s, F32)
        dm, line, half = pl.pallas_call(
            functools.partial(kernel, sizes),
            out_shape=(vm(nx, ny, nz), vm(nx, ny), vm(1, 128)),
            in_specs=[pl.BlockSpec(memory_space=pl.ANY)] * 2,
            out_specs=(pl.BlockSpec(memory_space=pl.ANY),) + (pl.BlockSpec(memory_space=pltpu.VMEM),) * 2,
            scratch_shapes=[
                vm(6, 2, nx + 4, PITCH, 128),
                vm(6, 16, 128),
                vm(2, 9, 2, nx, 128),
                vm(2, 9, 2, nx, 128),
                vm(4, 24, 128),
                vm(4, 24, 128),
                vm(2, 6, 16, 128),
                vm(6, 32, 128),
                vm(2, 8, 128),
                vm(3, 2, 8, 128),
                vm(2, 16, 128),
                vm(3, 2, 16, 128),
                vm(4, 2, 1, 128),
                vm(3, 4, 2, 1, 128),
                vm(4, 8, 128),
                vm(2, 16, 128),
                vm(12, 24, 128),
                vm(3, 24, 128),
                vm(12, 16, 128),
                vm(3, 24, 128),
                vm(3, 24, 128),
                vm(12, 2, 24, 128),
                vm(12, 2, nx + 4, 16, 128),
                vm(3, 2, nx + 4, 24, 128),
                vm(3, 2, nx + 4, 24, 128),
                vm(nx + 4, 2, 24, 128),
                vm(nx, 2, 16, 128),
                vm(2, nx, 16, 128),
                vm(2 * ngz, 8, 128),
                vm(ngx * ngy // 2, 1, 128),
                pltpu.SemaphoreType.DMA((6,)),
                pltpu.SemaphoreType.DMA((36 + 2 * ngz + ngx * ngy // 2,)),
                pltpu.SemaphoreType.DMA((36 + 2 * ngz + ngx * ngy // 2,)),
            ],
            compiler_params=pltpu.CompilerParams(collective_id=0, has_side_effects=True),
        )(velocity, metric)
        coefficient = jnp.minimum(line, half[0, 0])
        return coefficient[:, :, None] * dm, coefficient

    return jax.shard_map(
        per_device,
        mesh=mesh,
        in_specs=(P(None, "gx", "gy", "gz"), P(None, "gx", "gy", "gz")),
        out_specs=(P("gx", "gy", "gz"), P("gx", "gy")),
        check_vma=False,
    )
```

```python
import functools
import jax
import jax.numpy as jnp
from jax import lax
from jax.experimental import pallas as pl
from jax.experimental.pallas import tpu as pltpu
from jax.sharding import PartitionSpec as P

PAIRS = ((0, 0), (1, 1), (2, 2), (0, 1), (0, 2), (1, 2))
F32 = jnp.float32
MESH = pl.DeviceIdType.MESH
PITCH = 32
BASE = 8
UA, UY, UV, UC, UE4 = 2, 4, 7, 4, 4


def strain_of(diffs, m):
    g = [[m[j] * diffs[i][j] for j in range(3)] for i in range(3)]
    s = [g[a][a] if a == b else g[a][b] + g[b][a] for a, b in PAIRS]
    diag = s[0] * s[0] + s[1] * s[1] + s[2] * s[2]
    off = s[3] * s[3] + s[4] * s[4] + s[5] * s[5]
    return s, jnp.sqrt(0.5 * diag + 0.25 * off)


def kernel(sizes, vel, met, dm_out, line_out, half_out, U, O6, SY, RY, SC, RC, RO, ZG, SZX, RZX, SZY, RZY,
           SZC, RZC, ZC, SZG, TZ, UE, ZE, VE, VHE, T, YF, YV, VH, MB, DM, NP, LN, RX, lsem, ssem, rsem):
    ngx, ngy, ngz = sizes
    nx = vel.shape[1]
    ny = vel.shape[2]
    nz = vel.shape[3]
    gx, gy, gz = lax.axis_index("gx"), lax.axis_index("gy"), lax.axis_index("gz")
    has = {("x", 0): gx > 0, ("x", 1): gx < ngx - 1, ("y", 0): gy > 0, ("y", 1): gy < ngy - 1}

    ins = []
    for zt in range(2):
        for k, ref in enumerate((vel, met)):
            cp = pltpu.make_async_copy(
                ref.at[:, :, :, pl.ds(128 * zt, 128)],
                U.at[pl.ds(3 * k, 3), zt, pl.ds(2, nx), pl.ds(BASE, ny), :],
                lsem.at[2 * zt + k],
            )
            cp.start()
            ins.append(cp)

    bar = pltpu.get_barrier_semaphore()

    def greet(dev):
        pl.semaphore_signal(bar, inc=1, device_id=dev, device_id_type=MESH)

    def dx(s):
        return gx + (1 if s else -1)

    def dy(s):
        return gy + (1 if s else -1)

    def gz_at(d):
        return lax.rem(gz + d + ngz, ngz)

    both = {(sx, sy): jnp.logical_and(has["x", sx], has["y", sy]) for sx in range(2) for sy in range(2)}
    for d in (-1, 1):
        greet({"gz": gz_at(d)})
    for s in range(2):
        @pl.when(has["y", s])
        def _():
            for d in (-1, 0, 1):
                greet({"gy": dy(s), "gz": gz_at(d)})

        @pl.when(has["x", s])
        def _():
            for d in (-1, 0, 1):
                greet({"gx": dx(s), "gz": gz_at(d)})

        for q in range(2):
            @pl.when(both[s, q])
            def _():
                for d in (-1, 0, 1):
                    greet({"gx": dx(s), "gy": dy(q), "gz": gz_at(d)})

    core, xhi, nhi = lax.rem(gy, 2), lax.div(gy, 2), ngy // 2
    n1, n2 = 2 * ngz, ngx * nhi
    me1, me2 = core * ngz + gz, gx * nhi + xhi

    def dev1(k):
        c = lax.rem(me1 + k, n1)
        return c, {"gy": 2 * xhi + lax.div(c, ngz), "gz": lax.rem(c, ngz)}

    def dev2(k):
        c = lax.rem(me2 + k, n2)
        return c, {"gx": lax.div(c, nhi), "gy": 2 * lax.rem(c, nhi) + core}

    for k in range(1, n1):
        greet(dev1(k)[1])
    for k in range(1, n2):
        greet(dev2(k)[1])
    ex = has["x", 0].astype(jnp.int32) + has["x", 1].astype(jnp.int32)
    ey = has["y", 0].astype(jnp.int32) + has["y", 1].astype(jnp.int32)
    partners = 3 * (1 + ex) * (1 + ey) - 1 + n1 - 1 + n2 - 1

    z8 = jnp.zeros((8, 128), F32)
    for s in range(2):
        @pl.when(jnp.logical_not(has["x", s]))
        def _():
            for f in range(6):
                for zt in range(2):
                    for X in ((nx + 2, nx + 3) if s else (0, 1)):
                        for r in range(0, ny, 8):
                            U[f, zt, X, BASE + r : BASE + r + 8, :] = z8
            for d in range(3):
                RZX[d, s] = jnp.zeros(RZX.shape[2:], F32)

        @pl.when(jnp.logical_not(has["y", s]))
        def _():
            RY[s] = jnp.zeros(RY.shape[1:], F32)
            for d in range(3):
                RZY[d, s] = jnp.zeros(RZY.shape[2:], F32)

        for q in range(2):
            @pl.when(jnp.logical_not(both[s, q]))
            def _():
                RC[2 * s + q] = jnp.zeros(RC.shape[1:], F32)
                for d in range(3):
                    RZC[d, 2 * s + q] = jnp.zeros(RZC.shape[2:], F32)

    for cp in ins:
        cp.wait()
    for s in range(2):
        for f in range(6):
            for k in range(2):
                if f >= 3 and k != s:
                    continue
                y = (ny - 2 + k) if s else k
                slab = 2 * f + k if f < 3 else 3 + f
                for zt in range(2):
                    SY[s, slab, zt, :, :] = U[f, zt, pl.ds(2, nx), BASE + y, :]

    pl.semaphore_wait(bar, partners)

    waits_send, waits_recv = [], {}

    def put(n, src, dst, dev, send_if=None, recv_if=None):
        cp = pltpu.make_async_remote_copy(
            src_ref=src, dst_ref=dst, send_sem=ssem.at[n], recv_sem=rsem.at[n],
            device_id=dev, device_id_type=MESH)
        if send_if is None:
            cp.start()
        else:
            pl.when(send_if)(cp.start)
        waits_send.append((cp, send_if))
        waits_recv[n] = (cp, recv_if)

    def got(n):
        cp, cond = waits_recv[n]
        if cond is None:
            cp.wait_recv()
        else:
            pl.when(cond)(cp.wait_recv)

    for s in range(2):
        put(2 + s, SY.at[s], RY.at[1 - s], {"gy": dy(s)}, has["y", s], has["y", 1 - s])

    lane = lax.broadcasted_iota(jnp.int32, (8, 128), 1)
    lx = lax.shift_right_logical(lane * 43, 8)
    lc = lane - 6 * lx
    row = lax.broadcasted_iota(jnp.int32, (8, 128), 0)
    half = lane < 64
    for f in range(6):
        for t in range(2):
            acc = z8
            rows = slice(BASE + 8 * t, BASE + 8 * t + 8)
            for X in range(2, nx + 2):
                a = jnp.where(half, U[f, 0, X, rows, :], U[f, 1, X, rows, :])
                acc = jnp.where(lx == X, pltpu.roll(a, (6 * X + 2) % 128, 1), acc)
            O6[f, 8 * t : 8 * t + 8, :] = acc

    def x_at(f, t):
        return 54 * t + (12 * f if f < 3 else 18 + 6 * f)

    def x_lanes(lanes, at, f):
        return jnp.logical_and(lanes >= at, lanes < at + (12 if f < 3 else 6))

    for s in range(2):
        acc = z8
        for t in range(2):
            for f in range(6):
                first = 6 * ((nx + (f >= 3)) if s else 2)
                part = pltpu.roll(O6[f, 8 * t : 8 * t + 8, :], (x_at(f, t) - first) % 128, 1)
                acc = jnp.where(x_lanes(lane, x_at(f, t), f), part, acc)
        SZX[s] = acc
        for sy in range(2):
            for k in range(2):
                SZC[2 * s + sy, k] = acc[6 + k : 7 + k] if sy else acc[k : k + 1]
        y = ny - 2 if s else 0
        for f in range(6):
            SZY[s, 2 * f : 2 * f + 2, :] = O6[f, y : y + 2, :]
        SZY[s, 12:16, :] = z8[0:4]

    def corner_rows(sx, sy):
        rows = [(f, kx, ky) for f in range(6) for kx in range(2) for ky in range(2)
                if (kx == sx and ky == sy) or (f < 3 and (kx == sx or ky == sy))]
        return [(12 * zt + r, zt, *q) for zt in range(2) for r, q in enumerate(rows)]

    for sx in range(2):
        for sy in range(2):
            for r, zt, f, kx, ky in corner_rows(sx, sy):
                X, yr = (nx if sx else 2) + kx, (ny - 2 if sy else 0) + ky + BASE
                SC[2 * sx + sy, r : r + 1, :] = U[f, zt, X, yr : yr + 1, :]

    for s in range(2):
        put(s, O6, RO.at[1 - s], {"gz": gz_at(1 if s else -1)})
    for i, d in enumerate((-1, 0, 1)):
        o = 2 - i
        for s in range(2):
            put(12 + 2 * i + s, SZY.at[s], RZY.at[o, 1 - s], {"gy": dy(s), "gz": gz_at(d)},
                has["y", s], has["y", 1 - s])
            put(18 + 2 * i + s, SZX.at[s], RZX.at[o, 1 - s], {"gx": dx(s), "gz": gz_at(d)},
                has["x", s], has["x", 1 - s])
        for sx in range(2):
            for sy in range(2):
                put(24 + 4 * i + 2 * sx + sy, SZC.at[2 * sx + sy],
                    RZC.at[o, 2 * (1 - sx) + 1 - sy],
                    {"gx": dx(sx), "gy": dy(sy), "gz": gz_at(d)},
                    both[sx, sy], both[1 - sx, 1 - sy])
    for sx in range(2):
        for sy in range(2):
            put(8 + 2 * sx + sy, SC.at[2 * sx + sy], RC.at[2 * (1 - sx) + 1 - sy],
                {"gx": dx(sx), "gy": dy(sy)}, both[sx, sy], both[1 - sx, 1 - sy])
    def comb(left, own, right):
        return jnp.where(lc < 2, left, jnp.where(lc == 2, own, pltpu.roll(jnp.where(lc == 1, own, right), 2, 1)))

    got(0)
    got(1)
    for n in (12,13,14,15,16,17):
        got(n)
    rr = pl.ds(BASE, ny)
    for s in range(2):
        far, near = (nx, nx + 1) if s else (3, 2)
        gfar, gnear = (0, 1) if s else (nx + 3, nx + 2)
        put(4 + s, U.at[:, :, near, rr, :], U.at[:, :, gnear, rr, :], {"gx": dx(s)},
            has["x", s], has["x", 1 - s])
        put(6 + s, U.at[pl.ds(0, 3), :, far, rr, :], U.at[pl.ds(0, 3), :, gfar, rr, :],
            {"gx": dx(s)}, has["x", s], has["x", 1 - s])
    for n in range(18, 36):
        got(n)
    zx = [comb(RZX[0, s], RZX[1, s], RZX[2, s]) for s in range(2)]
    for s in range(2):
        for t in range(2):
            rows = slice(8 * t, 8 * t + 8)
            SZG[s, rows, :] = comb(RZY[0, s, rows, :], RZY[1, s, rows, :], RZY[2, s, rows, :])
    lane1 = lc[0:1]
    for c in range(4):
        ZC[c] = z8
        for k in range(2):
            left, own, right = (RZC[d, c, k] for d in range(3))
            ZC[c, k : k + 1, :] = jnp.where(lane1 < 2, left, jnp.where(
                lane1 == 2, own, pltpu.roll(jnp.where(lane1 == 1, own, right), 2, 1)))

    def x_place(sx, f):
        return 6 * (nx + 2) if sx else (0 if f < 3 else 6)

    for f in range(6):
        ZG[f, 0:8, :] = z8
        ZG[f, 24:32, :] = z8
        for t in range(2):
            rows = slice(8 * t, 8 * t + 8)
            z = comb(RO[0, f, rows, :], O6[f, rows, :], RO[1, f, rows, :])
            for sx in range(2):
                at = x_place(sx, f)
                part = pltpu.roll(zx[sx], (at - x_at(f, t)) % 128, 1)
                z = jnp.where(x_lanes(lane, at, f), part, z)
            ZG[f, BASE + 8 * t : BASE + 8 * t + 8, :] = z
        for sy in range(2):
            yr = BASE + (ny if sy else -2)
            z = SZG[sy, 2 * f : 2 * f + 2, :]
            for sx in range(2):
                at = x_place(sx, f)
                part = pltpu.roll(ZC[2 * sx + sy], (at - x_at(f, 1 - sy)) % 128, 1)[0:2]
                z = jnp.where(x_lanes(lane[0:2], at, f), part, z)
            ZG[f, yr : yr + 2, :] = z

    def edge(a):
        return jnp.where(lc == 0, pltpu.roll(a, 124, 1), a)

    def xsum(a):
        return pltpu.roll(a, 6, 1) + 2.0 * a + pltpu.roll(a, 122, 1)

    xd = lambda a: pltpu.roll(a, 122, 1) - pltpu.roll(a, 6, 1)
    zd = lambda a: pltpu.roll(a, 127, 1) - pltpu.roll(a, 1, 1)
    for t in range(3):
        r0 = BASE - 1 + 8 * t
        at = lambda f, d: ZG[f, r0 + d : r0 + d + 8, :]
        u = [at(i, 0) for i in range(3)]
        up = [at(i, 1) for i in range(3)]
        dn = [at(i, -1) for i in range(3)]
        m = [at(3 + j, 0) for j in range(3)]
        d = [[xd(u[i]), up[i] - dn[i], zd(u[i])] for i in range(3)]
        s, mag = strain_of(d, m)
        for p, (a, b) in enumerate(PAIRS):
            TZ[p, 8 * t : 8 * t + 8, :] = u[a] * u[b]
            TZ[6 + p, 8 * t : 8 * t + 8, :] = (0.5 if a == b else 0.25) * mag * s[p]
        for i in range(3):
            UE[i, 8 * t : 8 * t + 8, :] = edge(u[i])
            v = xsum(up[i] + dn[i] + 2.0 * u[i])
            VE[i, 8 * t : 8 * t + 8, :] = edge(v)
            vz = (1.0 / 64.0) * (pltpu.roll(v, 1, 1) + 2.0 * v + pltpu.roll(v, 127, 1))
            VHE[i, 8 * t : 8 * t + 8, :] = edge(vz)
    for p in range(12):
        for t in range(2):
            a = TZ[p, 8 * t : 8 * t + 8, :] + 2.0 * TZ[p, 8 * t + 1 : 8 * t + 9, :] + TZ[p, 8 * t + 2 : 8 * t + 10, :]
            ZE[p, 8 * t : 8 * t + 8, :] = edge(xsum(a))

    first_lane, last_lane = lane == 0, lane == 127

    def zshift(a, e):
        p0, p1 = pltpu.roll(a[0], 1, 1), pltpu.roll(a[1], 1, 1)
        n0, n1 = pltpu.roll(a[0], 127, 1), pltpu.roll(a[1], 127, 1)
        prev = (jnp.where(first_lane, e, p0), jnp.where(first_lane, p0, p1))
        nxt = (jnp.where(last_lane, n1, n0), jnp.where(last_lane, e, n1))
        return prev, nxt

    def stage_a(X, _):
        turn = 127 - 6 * X
        for t in range(3):
            r0 = BASE - 1 + 8 * t
            u = [[U[i, zt, X, r0 : r0 + 8, :] for zt in range(2)] for i in range(3)]
            zs = [zshift(u[i], pltpu.roll(UE[i, 8 * t : 8 * t + 8, :], turn, 1)) for i in range(3)]
            for zt in range(2):
                d = []
                for i in range(3):
                    ddx = U[i, zt, X + 1, r0 : r0 + 8, :] - U[i, zt, X - 1, r0 : r0 + 8, :]
                    ddy = U[i, zt, X, r0 + 1 : r0 + 9, :] - U[i, zt, X, r0 - 1 : r0 + 7, :]
                    d.append([ddx, ddy, zs[i][1][zt] - zs[i][0][zt]])
                m = [U[3 + j, zt, X, r0 : r0 + 8, :] for j in range(3)]
                s, mag = strain_of(d, m)
                for p, (a, b) in enumerate(PAIRS):
                    T[p, zt, 8 * t : 8 * t + 8, :] = u[a][zt] * u[b][zt]
                    T[6 + p, zt, 8 * t : 8 * t + 8, :] = (0.5 if a == b else 0.25) * mag * s[p]
                MB[X, zt, 8 * t : 8 * t + 8, :] = mag
        for p in range(12):
            for zt in range(2):
                for t in range(2):
                    r = 8 * t
                    YF[p, zt, X, r : r + 8, :] = (
                        T[p, zt, r : r + 8, :] + 2.0 * T[p, zt, r + 1 : r + 9, :] + T[p, zt, r + 2 : r + 10, :])
        return 0


    def stage_y(X, _):
        for i in range(3):
            for zt in range(2):
                for t in range(3):
                    r = BASE - 1 + 8 * t
                    YV[i, zt, X, 8 * t : 8 * t + 8, :] = (
                        U[i, zt, X, r - 1 : r + 7, :] + 2.0 * U[i, zt, X, r : r + 8, :] + U[i, zt, X, r + 1 : r + 9, :])
        return 0


    def stage_v(X, _):
        turn = 127 - 6 * X
        x_in = jnp.logical_and(jnp.logical_or(X >= 2, gx > 0), jnp.logical_or(X < nx + 2, gx < ngx - 1))
        for t in range(3):
            rr_ = row + 8 * t
            y_in = jnp.logical_and(rr_ >= jnp.where(gy > 0, 0, 1), rr_ < jnp.where(gy < ngy - 1, ny + 2, ny + 1))
            inside = jnp.logical_and(y_in, x_in)
            for i in range(3):
                a = [YV[i, zt, X - 1, 8 * t : 8 * t + 8, :] + 2.0 * YV[i, zt, X, 8 * t : 8 * t + 8, :]
                     + YV[i, zt, X + 1, 8 * t : 8 * t + 8, :] for zt in range(2)]
                prev, nxt = zshift(a, pltpu.roll(VE[i, 8 * t : 8 * t + 8, :], turn, 1))
                for zt in range(2):
                    v = (1.0 / 64.0) * (prev[zt] + 2.0 * a[zt] + nxt[zt])
                    VH[i, zt, X, 8 * t : 8 * t + 8, :] = jnp.where(inside, v, 0.0)
        return 0


    def stage_c(X, _):
        turn = 127 - 6 * X
        for t in range(2):
            r = 8 * t
            v = [[VH[i, zt, X, r + 1 : r + 9, :] for zt in range(2)] for i in range(3)]
            zs = [zshift(v[i], pltpu.roll(VHE[i, r + 1 : r + 9, :], turn, 1)) for i in range(3)]
            fl = []
            for p in range(12):
                a = [YF[p, zt, X - 1, r : r + 8, :] + 2.0 * YF[p, zt, X, r : r + 8, :]
                     + YF[p, zt, X + 1, r : r + 8, :] for zt in range(2)]
                prev, nxt = zshift(a, pltpu.roll(ZE[p, r : r + 8, :], turn, 1))
                fl.append([(1.0 / 64.0) * (prev[zt] + 2.0 * a[zt] + nxt[zt]) for zt in range(2)])
            num = den = None
            for zt in range(2):
                d = []
                for i in range(3):
                    ddx = VH[i, zt, X + 1, r + 1 : r + 9, :] - VH[i, zt, X - 1, r + 1 : r + 9, :]
                    ddy = VH[i, zt, X, r + 2 : r + 10, :] - VH[i, zt, X, r : r + 8, :]
                    d.append([ddx, ddy, zs[i][1][zt] - zs[i][0][zt]])
                m = [U[3 + j, zt, X, BASE + r : BASE + r + 8, :] for j in range(3)]
                s, mag = strain_of(d, m)
                delta = jnp.exp2((-2.0 / 3.0) * jnp.log2(m[0] * m[1] * m[2]))
                nn = dd = None
                for p, (a, b) in enumerate(PAIRS):
                    w = 1.0 if a == b else 2.0
                    leo = fl[p][zt] - v[a][zt] * v[b][zt]
                    q = fl[6 + p][zt] - (2.0 if a == b else 1.0) * mag * s[p]
                    wq = q if a == b else w * q
                    n_, d_ = wq * leo, wq * q
                    nn = n_ if nn is None else nn + n_
                    dd = d_ if dd is None else dd + d_
                d2 = 2.0 * delta
                n_, d_ = d2 * nn, d2 * d2 * dd
                num = n_ if num is None else num + n_
                den = d_ if den is None else den + d_
                DM[X - 2, zt, r : r + 8, :] = delta * MB[X, zt, r + 1 : r + 9, :]
            NP[0, X - 2, r : r + 8, :] = num
            NP[1, X - 2, r : r + 8, :] = den
        return 0

    def line_sums(acc, planes):
        for x in planes:
            for t in range(2):
                for k in range(2):
                    part = jnp.sum(NP[k, x, 8 * t : 8 * t + 8, :], axis=1, keepdims=True)
                    acc = jnp.where(lane == x + nx * t + 2 * nx * k, part, acc)
        return acc

    got(2)
    got(3)

    for s in range(2):
        for f in range(6):
            for k in range(2):
                if f >= 3 and k == s:
                    continue
                y = (ny + k) if s else k - 2
                slab = 2 * f + k if f < 3 else 3 + f
                for zt in range(2):
                    U[f, zt, pl.ds(2, nx), BASE + y, :] = RY[s, slab, zt, :, :]
    lax.fori_loop(3, nx + 1, stage_a, 0, unroll=UA)
    lax.fori_loop(2, nx + 2, stage_y, 0, unroll=UY)
    lax.fori_loop(3, nx + 1, stage_v, 0, unroll=UV)
    lax.fori_loop(4, nx, stage_c, 0, unroll=UC)

    sums = line_sums(z8, range(2, nx - 2))

    for n in range(8, 12):
        got(n)
    for sx in range(2):
        for sy in range(2):
            for r, zt, f, kx, ky in corner_rows(1 - sx, 1 - sy):
                X, yr = (nx + 2 if sx else 0) + kx, (ny if sy else -2) + ky + BASE
                U[f, zt, X, yr : yr + 1, :] = RC[2 * sx + sy, r : r + 1, :]

    for n in range(4, 8):
        got(n)
    def ends(a, stage):
        lax.fori_loop(0, 4, lambda k, c: stage(jnp.where(k < 2, a + k, nx - a + k), c), 0, unroll=UE4)

    ends(1, stage_a)
    ends(0, stage_y)
    ends(1, stage_v)
    ends(2, stage_c)
    LN[me1] = line_sums(sums, (0, 1, nx - 2, nx - 1))

    outs = []
    for zt in range(2):
        cp = pltpu.make_async_copy(DM.at[:, zt], dm_out.at[:, :, pl.ds(128 * zt, 128)], lsem.at[4 + zt])
        cp.start()
        outs.append(cp)

    cps = []

    def spread(ref, me, n, dev, at, order, meanwhile=None):
        def copy(k, c):
            return pltpu.make_async_remote_copy(
                src_ref=ref.at[me], dst_ref=ref.at[c], send_sem=ssem.at[at + k], recv_sem=rsem.at[at + c],
                device_id=dev(k)[1], device_id_type=MESH)

        for k in order:
            cp = copy(k, me)
            cp.start()
            cps.append(cp)
        if meanwhile is not None:
            meanwhile()
        for k in reversed(order):
            copy(k, dev(k)[0]).wait_recv()

    def far_first(n, span):
        return sorted(range(1, n), key=lambda k: -min(k % span, span - k % span))

    spread(LN, me1, n1, dev1, 36, far_first(n1, ngz))

    def line_of(q):
        tot = LN[q * ngz]
        for k in range(1, ngz):
            tot = tot + LN[q * ngz + k]
        tot = tot * (1.0 / (nz * ngz))
        return tot / (pltpu.roll(tot, 128 - 2 * nx, 1) + 1e-06)

    peak = jnp.where(lane < 2 * nx, jnp.maximum(line_of(0), line_of(1)), -jnp.inf)
    peak = jnp.max(jnp.max(peak, axis=0, keepdims=True), axis=1, keepdims=True)

    RX[me2] = jnp.broadcast_to(peak, (1, 128))

    def while_peak_travels():
        lt = line_of(core).T
        for t in range(2):
            line_out[:, 8 * t : 8 * t + 8] = lt[nx * t : nx * t + nx, :]
        for cp in outs:
            cp.wait()
        for cp in cps:
            cp.wait_send()
        for cp, cond in waits_send:
            if cond is None:
                cp.wait_send()
            else:
                pl.when(cond)(cp.wait_send)

    spread(RX, me2, n2, dev2, 36 + n1, far_first(n2, n2), while_peak_travels)
    peak = RX[0]
    for k in range(1, n2):
        peak = jnp.maximum(peak, RX[k])
    half_out[...] = 0.5 * peak


def solution(mesh):
    sizes = tuple(mesh.shape[a] for a in ("gx", "gy", "gz"))
    ngx, ngy, ngz = sizes

    def per_device(velocity, metric):
        _, nx, ny, nz = velocity.shape
        vm = lambda *s: pltpu.VMEM(s, F32)
        dm, line, half = pl.pallas_call(
            functools.partial(kernel, sizes),
            out_shape=(vm(nx, ny, nz), vm(nx, ny), vm(1, 128)),
            in_specs=[pl.BlockSpec(memory_space=pl.ANY)] * 2,
            out_specs=(pl.BlockSpec(memory_space=pl.ANY),) + (pl.BlockSpec(memory_space=pltpu.VMEM),) * 2,
            scratch_shapes=[
                vm(6, 2, nx + 4, PITCH, 128),
                vm(6, 16, 128),
                vm(2, 9, 2, nx, 128),
                vm(2, 9, 2, nx, 128),
                vm(4, 24, 128),
                vm(4, 24, 128),
                vm(2, 6, 16, 128),
                vm(6, 32, 128),
                vm(2, 8, 128),
                vm(3, 2, 8, 128),
                vm(2, 16, 128),
                vm(3, 2, 16, 128),
                vm(4, 2, 1, 128),
                vm(3, 4, 2, 1, 128),
                vm(4, 8, 128),
                vm(2, 16, 128),
                vm(12, 24, 128),
                vm(3, 24, 128),
                vm(12, 16, 128),
                vm(3, 24, 128),
                vm(3, 24, 128),
                vm(12, 2, 24, 128),
                vm(12, 2, nx + 4, 16, 128),
                vm(3, 2, nx + 4, 24, 128),
                vm(3, 2, nx + 4, 24, 128),
                vm(nx + 4, 2, 24, 128),
                vm(nx, 2, 16, 128),
                vm(2, nx, 16, 128),
                vm(2 * ngz, 8, 128),
                vm(ngx * ngy // 2, 1, 128),
                pltpu.SemaphoreType.DMA((6,)),
                pltpu.SemaphoreType.DMA((36 + 2 * ngz + ngx * ngy // 2,)),
                pltpu.SemaphoreType.DMA((36 + 2 * ngz + ngx * ngy // 2,)),
            ],
            compiler_params=pltpu.CompilerParams(collective_id=0, has_side_effects=True),
        )(velocity, metric)
        coefficient = jnp.minimum(line, half[0, 0])
        return coefficient[:, :, None] * dm, coefficient

    return jax.shard_map(
        per_device,
        mesh=mesh,
        in_specs=(P(None, "gx", "gy", "gz"), P(None, "gx", "gy", "gz")),
        out_specs=(P("gx", "gy", "gz"), P("gx", "gy")),
        check_vma=False,
    )
```

```python
import functools
import jax
import jax.numpy as jnp
from jax import lax
from jax.experimental import pallas as pl
from jax.experimental.pallas import tpu as pltpu
from jax.sharding import PartitionSpec as P

PAIRS = ((0, 0), (1, 1), (2, 2), (0, 1), (0, 2), (1, 2))
F32 = jnp.float32
MESH = pl.DeviceIdType.MESH
PITCH = 32
BASE = 8
UA, UY, UV, UC, UE4 = 7, 4, 7, 6, 4


def strain_of(diffs, m):
    g = [[m[j] * diffs[i][j] for j in range(3)] for i in range(3)]
    s = [g[a][a] if a == b else g[a][b] + g[b][a] for a, b in PAIRS]
    diag = s[0] * s[0] + s[1] * s[1] + s[2] * s[2]
    off = s[3] * s[3] + s[4] * s[4] + s[5] * s[5]
    return s, jnp.sqrt(0.5 * diag + 0.25 * off)


def kernel(sizes, vel, met, dm_out, line_out, half_out, U, O6, SY, RY, SC, RC, RO, ZG, SZX, RZX, SZY, RZY,
           SZC, RZC, ZC, SZG, TZ, UE, ZE, VE, VHE, T, YF, YV, VH, MB, DM, NP, LN, RX, lsem, ssem, rsem):
    ngx, ngy, ngz = sizes
    nx = vel.shape[1]
    ny = vel.shape[2]
    nz = vel.shape[3]
    gx, gy, gz = lax.axis_index("gx"), lax.axis_index("gy"), lax.axis_index("gz")
    has = {("x", 0): gx > 0, ("x", 1): gx < ngx - 1, ("y", 0): gy > 0, ("y", 1): gy < ngy - 1}

    ins = []
    for zt in range(2):
        for k, ref in enumerate((vel, met)):
            cp = pltpu.make_async_copy(
                ref.at[:, :, :, pl.ds(128 * zt, 128)],
                U.at[pl.ds(3 * k, 3), zt, pl.ds(2, nx), pl.ds(BASE, ny), :],
                lsem.at[2 * zt + k],
            )
            cp.start()
            ins.append(cp)

    bar = pltpu.get_barrier_semaphore()

    def greet(dev):
        pl.semaphore_signal(bar, inc=1, device_id=dev, device_id_type=MESH)

    def dx(s):
        return gx + (1 if s else -1)

    def dy(s):
        return gy + (1 if s else -1)

    def gz_at(d):
        return lax.rem(gz + d + ngz, ngz)

    both = {(sx, sy): jnp.logical_and(has["x", sx], has["y", sy]) for sx in range(2) for sy in range(2)}
    for d in (-1, 1):
        greet({"gz": gz_at(d)})
    for s in range(2):
        @pl.when(has["y", s])
        def _():
            for d in (-1, 0, 1):
                greet({"gy": dy(s), "gz": gz_at(d)})

        @pl.when(has["x", s])
        def _():
            for d in (-1, 0, 1):
                greet({"gx": dx(s), "gz": gz_at(d)})

        for q in range(2):
            @pl.when(both[s, q])
            def _():
                for d in (-1, 0, 1):
                    greet({"gx": dx(s), "gy": dy(q), "gz": gz_at(d)})

    core, xhi, nhi = lax.rem(gy, 2), lax.div(gy, 2), ngy // 2
    n1, n2 = 2 * ngz, ngx * nhi
    me1, me2 = core * ngz + gz, gx * nhi + xhi

    def dev1(k):
        c = lax.rem(me1 + k, n1)
        return c, {"gy": 2 * xhi + lax.div(c, ngz), "gz": lax.rem(c, ngz)}

    def dev2(k):
        c = lax.rem(me2 + k, n2)
        return c, {"gx": lax.div(c, nhi), "gy": 2 * lax.rem(c, nhi) + core}

    for k in range(1, n1):
        greet(dev1(k)[1])
    for k in range(1, n2):
        greet(dev2(k)[1])
    ex = has["x", 0].astype(jnp.int32) + has["x", 1].astype(jnp.int32)
    ey = has["y", 0].astype(jnp.int32) + has["y", 1].astype(jnp.int32)
    partners = 3 * (1 + ex) * (1 + ey) - 1 + n1 - 1 + n2 - 1

    z8 = jnp.zeros((8, 128), F32)
    for s in range(2):
        @pl.when(jnp.logical_not(has["x", s]))
        def _():
            for f in range(6):
                for zt in range(2):
                    for X in ((nx + 2, nx + 3) if s else (0, 1)):
                        for r in range(0, ny, 8):
                            U[f, zt, X, BASE + r : BASE + r + 8, :] = z8
            for d in range(3):
                RZX[d, s] = jnp.zeros(RZX.shape[2:], F32)

        @pl.when(jnp.logical_not(has["y", s]))
        def _():
            RY[s] = jnp.zeros(RY.shape[1:], F32)
            for d in range(3):
                RZY[d, s] = jnp.zeros(RZY.shape[2:], F32)

        for q in range(2):
            @pl.when(jnp.logical_not(both[s, q]))
            def _():
                RC[2 * s + q] = jnp.zeros(RC.shape[1:], F32)
                for d in range(3):
                    RZC[d, 2 * s + q] = jnp.zeros(RZC.shape[2:], F32)

    for cp in ins:
        cp.wait()
    for s in range(2):
        for f in range(6):
            for k in range(2):
                if f >= 3 and k != s:
                    continue
                y = (ny - 2 + k) if s else k
                slab = 2 * f + k if f < 3 else 3 + f
                for zt in range(2):
                    SY[s, slab, zt, :, :] = U[f, zt, pl.ds(2, nx), BASE + y, :]

    pl.semaphore_wait(bar, partners)

    waits_send, waits_recv = [], {}

    def put(n, src, dst, dev, send_if=None, recv_if=None):
        cp = pltpu.make_async_remote_copy(
            src_ref=src, dst_ref=dst, send_sem=ssem.at[n], recv_sem=rsem.at[n],
            device_id=dev, device_id_type=MESH)
        if send_if is None:
            cp.start()
        else:
            pl.when(send_if)(cp.start)
        waits_send.append((cp, send_if))
        waits_recv[n] = (cp, recv_if)

    def got(n):
        cp, cond = waits_recv[n]
        if cond is None:
            cp.wait_recv()
        else:
            pl.when(cond)(cp.wait_recv)

    for s in range(2):
        put(2 + s, SY.at[s], RY.at[1 - s], {"gy": dy(s)}, has["y", s], has["y", 1 - s])

    lane = lax.broadcasted_iota(jnp.int32, (8, 128), 1)
    lx = lax.shift_right_logical(lane * 43, 8)
    lc = lane - 6 * lx
    row = lax.broadcasted_iota(jnp.int32, (8, 128), 0)
    half = lane < 64
    for f in range(6):
        for t in range(2):
            acc = z8
            rows = slice(BASE + 8 * t, BASE + 8 * t + 8)
            for X in range(2, nx + 2):
                a = jnp.where(half, U[f, 0, X, rows, :], U[f, 1, X, rows, :])
                acc = jnp.where(lx == X, pltpu.roll(a, (6 * X + 2) % 128, 1), acc)
            O6[f, 8 * t : 8 * t + 8, :] = acc

    def x_at(f, t):
        return 54 * t + (12 * f if f < 3 else 18 + 6 * f)

    def x_lanes(lanes, at, f):
        return jnp.logical_and(lanes >= at, lanes < at + (12 if f < 3 else 6))

    for s in range(2):
        acc = z8
        for t in range(2):
            for f in range(6):
                first = 6 * ((nx + (f >= 3)) if s else 2)
                part = pltpu.roll(O6[f, 8 * t : 8 * t + 8, :], (x_at(f, t) - first) % 128, 1)
                acc = jnp.where(x_lanes(lane, x_at(f, t), f), part, acc)
        SZX[s] = acc
        for sy in range(2):
            for k in range(2):
                SZC[2 * s + sy, k] = acc[6 + k : 7 + k] if sy else acc[k : k + 1]
        y = ny - 2 if s else 0
        for f in range(6):
            SZY[s, 2 * f : 2 * f + 2, :] = O6[f, y : y + 2, :]
        SZY[s, 12:16, :] = z8[0:4]

    def corner_rows(sx, sy):
        rows = [(f, kx, ky) for f in range(6) for kx in range(2) for ky in range(2)
                if (kx == sx and ky == sy) or (f < 3 and (kx == sx or ky == sy))]
        return [(12 * zt + r, zt, *q) for zt in range(2) for r, q in enumerate(rows)]

    for sx in range(2):
        for sy in range(2):
            for r, zt, f, kx, ky in corner_rows(sx, sy):
                X, yr = (nx if sx else 2) + kx, (ny - 2 if sy else 0) + ky + BASE
                SC[2 * sx + sy, r : r + 1, :] = U[f, zt, X, yr : yr + 1, :]

    for s in range(2):
        put(s, O6, RO.at[1 - s], {"gz": gz_at(1 if s else -1)})
    for i, d in enumerate((-1, 0, 1)):
        o = 2 - i
        for s in range(2):
            put(12 + 2 * i + s, SZY.at[s], RZY.at[o, 1 - s], {"gy": dy(s), "gz": gz_at(d)},
                has["y", s], has["y", 1 - s])
            put(18 + 2 * i + s, SZX.at[s], RZX.at[o, 1 - s], {"gx": dx(s), "gz": gz_at(d)},
                has["x", s], has["x", 1 - s])
        for sx in range(2):
            for sy in range(2):
                put(24 + 4 * i + 2 * sx + sy, SZC.at[2 * sx + sy],
                    RZC.at[o, 2 * (1 - sx) + 1 - sy],
                    {"gx": dx(sx), "gy": dy(sy), "gz": gz_at(d)},
                    both[sx, sy], both[1 - sx, 1 - sy])
    for sx in range(2):
        for sy in range(2):
            put(8 + 2 * sx + sy, SC.at[2 * sx + sy], RC.at[2 * (1 - sx) + 1 - sy],
                {"gx": dx(sx), "gy": dy(sy)}, both[sx, sy], both[1 - sx, 1 - sy])
    def comb(left, own, right):
        return jnp.where(lc < 2, left, jnp.where(lc == 2, own, pltpu.roll(jnp.where(lc == 1, own, right), 2, 1)))

    got(0)
    got(1)
    for n in (12,13,14,15,16,17):
        got(n)
    rr = pl.ds(BASE, ny)
    for s in range(2):
        far, near = (nx, nx + 1) if s else (3, 2)
        gfar, gnear = (0, 1) if s else (nx + 3, nx + 2)
        put(4 + s, U.at[:, :, near, rr, :], U.at[:, :, gnear, rr, :], {"gx": dx(s)},
            has["x", s], has["x", 1 - s])
        put(6 + s, U.at[pl.ds(0, 3), :, far, rr, :], U.at[pl.ds(0, 3), :, gfar, rr, :],
            {"gx": dx(s)}, has["x", s], has["x", 1 - s])
    for n in range(18, 36):
        got(n)
    zx = [comb(RZX[0, s], RZX[1, s], RZX[2, s]) for s in range(2)]
    for s in range(2):
        for t in range(2):
            rows = slice(8 * t, 8 * t + 8)
            SZG[s, rows, :] = comb(RZY[0, s, rows, :], RZY[1, s, rows, :], RZY[2, s, rows, :])
    lane1 = lc[0:1]
    for c in range(4):
        ZC[c] = z8
        for k in range(2):
            left, own, right = (RZC[d, c, k] for d in range(3))
            ZC[c, k : k + 1, :] = jnp.where(lane1 < 2, left, jnp.where(
                lane1 == 2, own, pltpu.roll(jnp.where(lane1 == 1, own, right), 2, 1)))

    def x_place(sx, f):
        return 6 * (nx + 2) if sx else (0 if f < 3 else 6)

    for f in range(6):
        ZG[f, 0:8, :] = z8
        ZG[f, 24:32, :] = z8
        for t in range(2):
            rows = slice(8 * t, 8 * t + 8)
            z = comb(RO[0, f, rows, :], O6[f, rows, :], RO[1, f, rows, :])
            for sx in range(2):
                at = x_place(sx, f)
                part = pltpu.roll(zx[sx], (at - x_at(f, t)) % 128, 1)
                z = jnp.where(x_lanes(lane, at, f), part, z)
            ZG[f, BASE + 8 * t : BASE + 8 * t + 8, :] = z
        for sy in range(2):
            yr = BASE + (ny if sy else -2)
            z = SZG[sy, 2 * f : 2 * f + 2, :]
            for sx in range(2):
                at = x_place(sx, f)
                part = pltpu.roll(ZC[2 * sx + sy], (at - x_at(f, 1 - sy)) % 128, 1)[0:2]
                z = jnp.where(x_lanes(lane[0:2], at, f), part, z)
            ZG[f, yr : yr + 2, :] = z

    def edge(a):
        return jnp.where(lc == 0, pltpu.roll(a, 124, 1), a)

    def xsum(a):
        return pltpu.roll(a, 6, 1) + 2.0 * a + pltpu.roll(a, 122, 1)

    xd = lambda a: pltpu.roll(a, 122, 1) - pltpu.roll(a, 6, 1)
    zd = lambda a: pltpu.roll(a, 127, 1) - pltpu.roll(a, 1, 1)
    for t in range(3):
        r0 = BASE - 1 + 8 * t
        at = lambda f, d: ZG[f, r0 + d : r0 + d + 8, :]
        u = [at(i, 0) for i in range(3)]
        up = [at(i, 1) for i in range(3)]
        dn = [at(i, -1) for i in range(3)]
        m = [at(3 + j, 0) for j in range(3)]
        d = [[xd(u[i]), up[i] - dn[i], zd(u[i])] for i in range(3)]
        s, mag = strain_of(d, m)
        for p, (a, b) in enumerate(PAIRS):
            TZ[p, 8 * t : 8 * t + 8, :] = u[a] * u[b]
            TZ[6 + p, 8 * t : 8 * t + 8, :] = (0.5 if a == b else 0.25) * mag * s[p]
        for i in range(3):
            UE[i, 8 * t : 8 * t + 8, :] = edge(u[i])
            v = xsum(up[i] + dn[i] + 2.0 * u[i])
            VE[i, 8 * t : 8 * t + 8, :] = edge(v)
            vz = (1.0 / 64.0) * (pltpu.roll(v, 1, 1) + 2.0 * v + pltpu.roll(v, 127, 1))
            VHE[i, 8 * t : 8 * t + 8, :] = edge(vz)
    for p in range(12):
        for t in range(2):
            a = TZ[p, 8 * t : 8 * t + 8, :] + 2.0 * TZ[p, 8 * t + 1 : 8 * t + 9, :] + TZ[p, 8 * t + 2 : 8 * t + 10, :]
            ZE[p, 8 * t : 8 * t + 8, :] = edge(xsum(a))

    first_lane, last_lane = lane == 0, lane == 127

    def zshift(a, e):
        p0, p1 = pltpu.roll(a[0], 1, 1), pltpu.roll(a[1], 1, 1)
        n0, n1 = pltpu.roll(a[0], 127, 1), pltpu.roll(a[1], 127, 1)
        prev = (jnp.where(first_lane, e, p0), jnp.where(first_lane, p0, p1))
        nxt = (jnp.where(last_lane, n1, n0), jnp.where(last_lane, e, n1))
        return prev, nxt

    def stage_a(X, _):
        turn = 127 - 6 * X
        for t in range(3):
            r0 = BASE - 1 + 8 * t
            u = [[U[i, zt, X, r0 : r0 + 8, :] for zt in range(2)] for i in range(3)]
            zs = [zshift(u[i], pltpu.roll(UE[i, 8 * t : 8 * t + 8, :], turn, 1)) for i in range(3)]
            for zt in range(2):
                d = []
                for i in range(3):
                    ddx = U[i, zt, X + 1, r0 : r0 + 8, :] - U[i, zt, X - 1, r0 : r0 + 8, :]
                    ddy = U[i, zt, X, r0 + 1 : r0 + 9, :] - U[i, zt, X, r0 - 1 : r0 + 7, :]
                    d.append([ddx, ddy, zs[i][1][zt] - zs[i][0][zt]])
                m = [U[3 + j, zt, X, r0 : r0 + 8, :] for j in range(3)]
                s, mag = strain_of(d, m)
                for p, (a, b) in enumerate(PAIRS):
                    T[p, zt, 8 * t : 8 * t + 8, :] = u[a][zt] * u[b][zt]
                    T[6 + p, zt, 8 * t : 8 * t + 8, :] = (0.5 if a == b else 0.25) * mag * s[p]
                MB[X, zt, 8 * t : 8 * t + 8, :] = mag
        for p in range(12):
            for zt in range(2):
                for t in range(2):
                    r = 8 * t
                    YF[p, zt, X, r : r + 8, :] = (
                        T[p, zt, r : r + 8, :] + 2.0 * T[p, zt, r + 1 : r + 9, :] + T[p, zt, r + 2 : r + 10, :])
        return 0


    def stage_y(X, _):
        for i in range(3):
            for zt in range(2):
                for t in range(3):
                    r = BASE - 1 + 8 * t
                    YV[i, zt, X, 8 * t : 8 * t + 8, :] = (
                        U[i, zt, X, r - 1 : r + 7, :] + 2.0 * U[i, zt, X, r : r + 8, :] + U[i, zt, X, r + 1 : r + 9, :])
        return 0


    def stage_v(X, _):
        turn = 127 - 6 * X
        x_in = jnp.logical_and(jnp.logical_or(X >= 2, gx > 0), jnp.logical_or(X < nx + 2, gx < ngx - 1))
        for t in range(3):
            rr_ = row + 8 * t
            y_in = jnp.logical_and(rr_ >= jnp.where(gy > 0, 0, 1), rr_ < jnp.where(gy < ngy - 1, ny + 2, ny + 1))
            inside = jnp.logical_and(y_in, x_in)
            for i in range(3):
                a = [YV[i, zt, X - 1, 8 * t : 8 * t + 8, :] + 2.0 * YV[i, zt, X, 8 * t : 8 * t + 8, :]
                     + YV[i, zt, X + 1, 8 * t : 8 * t + 8, :] for zt in range(2)]
                prev, nxt = zshift(a, pltpu.roll(VE[i, 8 * t : 8 * t + 8, :], turn, 1))
                for zt in range(2):
                    v = (1.0 / 64.0) * (prev[zt] + 2.0 * a[zt] + nxt[zt])
                    VH[i, zt, X, 8 * t : 8 * t + 8, :] = jnp.where(inside, v, 0.0)
        return 0


    def stage_c(X, _):
        turn = 127 - 6 * X
        for t in range(2):
            r = 8 * t
            v = [[VH[i, zt, X, r + 1 : r + 9, :] for zt in range(2)] for i in range(3)]
            zs = [zshift(v[i], pltpu.roll(VHE[i, r + 1 : r + 9, :], turn, 1)) for i in range(3)]
            fl = []
            for p in range(12):
                a = [YF[p, zt, X - 1, r : r + 8, :] + 2.0 * YF[p, zt, X, r : r + 8, :]
                     + YF[p, zt, X + 1, r : r + 8, :] for zt in range(2)]
                prev, nxt = zshift(a, pltpu.roll(ZE[p, r : r + 8, :], turn, 1))
                fl.append([(1.0 / 64.0) * (prev[zt] + 2.0 * a[zt] + nxt[zt]) for zt in range(2)])
            num = den = None
            for zt in range(2):
                d = []
                for i in range(3):
                    ddx = VH[i, zt, X + 1, r + 1 : r + 9, :] - VH[i, zt, X - 1, r + 1 : r + 9, :]
                    ddy = VH[i, zt, X, r + 2 : r + 10, :] - VH[i, zt, X, r : r + 8, :]
                    d.append([ddx, ddy, zs[i][1][zt] - zs[i][0][zt]])
                m = [U[3 + j, zt, X, BASE + r : BASE + r + 8, :] for j in range(3)]
                s, mag = strain_of(d, m)
                delta = jnp.exp2((-2.0 / 3.0) * jnp.log2(m[0] * m[1] * m[2]))
                nn = dd = None
                for p, (a, b) in enumerate(PAIRS):
                    w = 1.0 if a == b else 2.0
                    leo = fl[p][zt] - v[a][zt] * v[b][zt]
                    q = fl[6 + p][zt] - (2.0 if a == b else 1.0) * mag * s[p]
                    wq = q if a == b else w * q
                    n_, d_ = wq * leo, wq * q
                    nn = n_ if nn is None else nn + n_
                    dd = d_ if dd is None else dd + d_
                d2 = 2.0 * delta
                n_, d_ = d2 * nn, d2 * d2 * dd
                num = n_ if num is None else num + n_
                den = d_ if den is None else den + d_
                DM[X - 2, zt, r : r + 8, :] = delta * MB[X, zt, r + 1 : r + 9, :]
            NP[0, X - 2, r : r + 8, :] = num
            NP[1, X - 2, r : r + 8, :] = den
        return 0

    def line_sums(acc, planes):
        for x in planes:
            for t in range(2):
                for k in range(2):
                    part = jnp.sum(NP[k, x, 8 * t : 8 * t + 8, :], axis=1, keepdims=True)
                    acc = jnp.where(lane == x + nx * t + 2 * nx * k, part, acc)
        return acc

    got(2)
    got(3)

    for s in range(2):
        for f in range(6):
            for k in range(2):
                if f >= 3 and k == s:
                    continue
                y = (ny + k) if s else k - 2
                slab = 2 * f + k if f < 3 else 3 + f
                for zt in range(2):
                    U[f, zt, pl.ds(2, nx), BASE + y, :] = RY[s, slab, zt, :, :]
    lax.fori_loop(3, nx + 1, stage_a, 0, unroll=UA)
    lax.fori_loop(2, nx + 2, stage_y, 0, unroll=UY)
    lax.fori_loop(3, nx + 1, stage_v, 0, unroll=UV)
    lax.fori_loop(4, nx, stage_c, 0, unroll=UC)

    sums = line_sums(z8, range(2, nx - 2))

    for n in range(8, 12):
        got(n)
    for sx in range(2):
        for sy in range(2):
            for r, zt, f, kx, ky in corner_rows(1 - sx, 1 - sy):
                X, yr = (nx + 2 if sx else 0) + kx, (ny if sy else -2) + ky + BASE
                U[f, zt, X, yr : yr + 1, :] = RC[2 * sx + sy, r : r + 1, :]

    for n in range(4, 8):
        got(n)
    def ends(a, stage):
        lax.fori_loop(0, 4, lambda k, c: stage(jnp.where(k < 2, a + k, nx - a + k), c), 0, unroll=UE4)

    ends(1, stage_a)
    ends(0, stage_y)
    ends(1, stage_v)
    ends(2, stage_c)
    LN[me1] = line_sums(sums, (0, 1, nx - 2, nx - 1))

    outs = []
    for zt in range(2):
        cp = pltpu.make_async_copy(DM.at[:, zt], dm_out.at[:, :, pl.ds(128 * zt, 128)], lsem.at[4 + zt])
        cp.start()
        outs.append(cp)

    cps = []

    def spread(ref, me, n, dev, at, order, meanwhile=None):
        def copy(k, c):
            return pltpu.make_async_remote_copy(
                src_ref=ref.at[me], dst_ref=ref.at[c], send_sem=ssem.at[at + k], recv_sem=rsem.at[at + c],
                device_id=dev(k)[1], device_id_type=MESH)

        for k in order:
            cp = copy(k, me)
            cp.start()
            cps.append(cp)
        if meanwhile is not None:
            meanwhile()
        for k in reversed(order):
            copy(k, dev(k)[0]).wait_recv()

    def far_first(n, span):
        return sorted(range(1, n), key=lambda k: -min(k % span, span - k % span))

    spread(LN, me1, n1, dev1, 36, far_first(n1, ngz))

    def line_of(q):
        tot = LN[q * ngz]
        for k in range(1, ngz):
            tot = tot + LN[q * ngz + k]
        tot = tot * (1.0 / (nz * ngz))
        return tot / (pltpu.roll(tot, 128 - 2 * nx, 1) + 1e-06)

    peak = jnp.where(lane < 2 * nx, jnp.maximum(line_of(0), line_of(1)), -jnp.inf)
    peak = jnp.max(jnp.max(peak, axis=0, keepdims=True), axis=1, keepdims=True)

    RX[me2] = jnp.broadcast_to(peak, (1, 128))

    def while_peak_travels():
        lt = line_of(core).T
        for t in range(2):
            line_out[:, 8 * t : 8 * t + 8] = lt[nx * t : nx * t + nx, :]
        for cp in outs:
            cp.wait()
        for cp in cps:
            cp.wait_send()
        for cp, cond in waits_send:
            if cond is None:
                cp.wait_send()
            else:
                pl.when(cond)(cp.wait_send)

    spread(RX, me2, n2, dev2, 36 + n1, far_first(n2, n2), while_peak_travels)
    peak = RX[0]
    for k in range(1, n2):
        peak = jnp.maximum(peak, RX[k])
    half_out[...] = 0.5 * peak


def solution(mesh):
    sizes = tuple(mesh.shape[a] for a in ("gx", "gy", "gz"))
    ngx, ngy, ngz = sizes

    def per_device(velocity, metric):
        _, nx, ny, nz = velocity.shape
        vm = lambda *s: pltpu.VMEM(s, F32)
        dm, line, half = pl.pallas_call(
            functools.partial(kernel, sizes),
            out_shape=(vm(nx, ny, nz), vm(nx, ny), vm(1, 128)),
            in_specs=[pl.BlockSpec(memory_space=pl.ANY)] * 2,
            out_specs=(pl.BlockSpec(memory_space=pl.ANY),) + (pl.BlockSpec(memory_space=pltpu.VMEM),) * 2,
            scratch_shapes=[
                vm(6, 2, nx + 4, PITCH, 128),
                vm(6, 16, 128),
                vm(2, 9, 2, nx, 128),
                vm(2, 9, 2, nx, 128),
                vm(4, 24, 128),
                vm(4, 24, 128),
                vm(2, 6, 16, 128),
                vm(6, 32, 128),
                vm(2, 8, 128),
                vm(3, 2, 8, 128),
                vm(2, 16, 128),
                vm(3, 2, 16, 128),
                vm(4, 2, 1, 128),
                vm(3, 4, 2, 1, 128),
                vm(4, 8, 128),
                vm(2, 16, 128),
                vm(12, 24, 128),
                vm(3, 24, 128),
                vm(12, 16, 128),
                vm(3, 24, 128),
                vm(3, 24, 128),
                vm(12, 2, 24, 128),
                vm(12, 2, nx + 4, 16, 128),
                vm(3, 2, nx + 4, 24, 128),
                vm(3, 2, nx + 4, 24, 128),
                vm(nx + 4, 2, 24, 128),
                vm(nx, 2, 16, 128),
                vm(2, nx, 16, 128),
                vm(2 * ngz, 8, 128),
                vm(ngx * ngy // 2, 1, 128),
                pltpu.SemaphoreType.DMA((6,)),
                pltpu.SemaphoreType.DMA((36 + 2 * ngz + ngx * ngy // 2,)),
                pltpu.SemaphoreType.DMA((36 + 2 * ngz + ngx * ngy // 2,)),
            ],
            compiler_params=pltpu.CompilerParams(collective_id=0, has_side_effects=True),
        )(velocity, metric)
        coefficient = jnp.minimum(line, half[0, 0])
        return coefficient[:, :, None] * dm, coefficient

    return jax.shard_map(
        per_device,
        mesh=mesh,
        in_specs=(P(None, "gx", "gy", "gz"), P(None, "gx", "gy", "gz")),
        out_specs=(P("gx", "gy", "gz"), P("gx", "gy")),
        check_vma=False,
    )
```
